512 devices in a mesh: dp: 8 (over z_lo), row: 16 (over z_hi, x, core), col: 4 (over y).
Axes of the slice: x: 4, y: 4, z: 16 (z_hi: 2, z_lo: 8; z = z_hi * 8 + z_lo), core: 2. Of those that a mesh axis runs over, the one named last changes fastest.
Arguments:
- expand_gradient: bfloat16 [8, 4096, 5120], P('dp', 'row', 'col'), may hold values from -24 to 24, as said below
- expand_master: float32 [4096, 5120], P(('row', 'dp'), 'col'), may hold values from -0.12 to 0.12
- expand_rows: float32 [4096], P(('row', 'dp')), may hold values from 0.01 to 1
- expand_columns: float32 [5120], P('col'), may hold values from 0.01 to 1
- contract_gradient: bfloat16 [8, 5120, 4096], P('dp', 'row', 'col'), may hold values from -24 to 24, as said below
- contract_master: float32 [5120, 4096], P(('row', 'dp'), 'col'), may hold values from -0.12 to 0.12
- contract_rows: float32 [5120], P(('row', 'dp')), may hold values from 0.01 to 1
- contract_columns: float32 [4096], P('col'), may hold values from 0.01 to 1
- attend_gradient: bfloat16 [8, 4096, 4096], P('dp', 'row', 'col'), may hold values from -24 to 24, as said below
- attend_master: float32 [4096, 4096], P(('row', 'dp'), 'col'), may hold values from -0.12 to 0.12
- attend_rows: float32 [4096], P(('row', 'dp')), may hold values from 0.01 to 1
- attend_columns: float32 [4096], P('col'), may hold values from 0.01 to 1
Outputs:
- expand_updated: float32 [4096, 5120], P(('row', 'dp'), 'col')
- expand_weights: bfloat16 [4096, 5120], P('row', 'col')
- expand_rows_next: float32 [4096], P(('row', 'dp'))
- expand_columns_next: float32 [5120], P('col')
- expand_step: float32 [4096, 5120], P(('row', 'dp'), 'col')
- contract_updated: float32 [5120, 4096], P(('row', 'dp'), 'col')
- contract_weights: bfloat16 [5120, 4096], P('row', 'col')
- contract_rows_next: float32 [5120], P(('row', 'dp'))
- contract_columns_next: float32 [4096], P('col')
- contract_step: float32 [5120, 4096], P(('row', 'dp'), 'col')
- attend_updated: float32 [4096, 4096], P(('row', 'dp'), 'col')
- attend_weights: bfloat16 [4096, 4096], P('row', 'col')
- attend_rows_next: float32 [4096], P(('row', 'dp'))
- attend_columns_next: float32 [4096], P('col')
- attend_step: float32 [4096, 4096], P(('row', 'dp'), 'col')
The draws below stay inside these ranges and needn't reach their ends.
Inputs may be any that keep to these rules, and one draw needn't show every extreme that they name: `expand_gradient`: each replica's gradient, of any scale from entry to entry. `contract_gradient`: each replica's gradient, of any scale from entry to entry. `attend_gradient`: each replica's gradient, of any scale from entry to entry.
All inputs are finite; a program needn't handle non-finite values.
Results may differ from the reference program's by a relative error of at most 0.0004.
Values may be sent and summed in bfloat16 or wider, within the bound.
A program may use at most 64 MiB of HBM per device.

```python
import math
import jax
import jax.numpy as jnp
from jax import lax

D = 4096
FF = 5120
INNER = 4096
REPLICAS = 8


def scale_field(key, height, width):
    row_pos = jnp.arange(height, dtype=jnp.float32) / height
    col_pos = jnp.arange(width, dtype=jnp.float32) / width
    logs = jnp.zeros((height, width), jnp.float32)
    for term in range(3):
        sub = jax.random.fold_in(key, 100 + term)
        freq_keys = jax.random.split(sub, 4)
        row_freq = jax.random.randint(freq_keys[0], (), 1, 5).astype(jnp.float32)
        col_freq = jax.random.randint(freq_keys[1], (), 1, 4).astype(jnp.float32)
        row_phase = jax.random.uniform(freq_keys[2], (), jnp.float32, 0.0, 2.0 * math.pi)
        col_phase = jax.random.uniform(freq_keys[3], (), jnp.float32, 0.0, 2.0 * math.pi)
        along_rows = jnp.cos(2.0 * math.pi * row_freq * row_pos + row_phase)
        along_cols = jnp.cos(2.0 * math.pi * col_freq * col_pos + col_phase)
        logs = logs + 0.6 * along_rows[:, None] * along_cols[None, :]
    return jnp.exp(logs)


def gradient_draw(key, replicas, height, width):
    field = scale_field(jax.random.fold_in(key, 7), height, width)
    noise_key = jax.random.fold_in(key, 11)
    noise = jax.random.normal(noise_key, (replicas, height, width), jnp.float32)
    values = jnp.clip(2.0 * noise * field[None, :, :], -24.0, 24.0)
    return values.astype(jnp.bfloat16)


def draw_expand_gradient(key, part):
    return gradient_draw(jax.random.fold_in(key, 1), REPLICAS, D, FF)


def draw_contract_gradient(key, part):
    return gradient_draw(jax.random.fold_in(key, 2), REPLICAS, FF, D)


def draw_attend_gradient(key, part):
    return gradient_draw(jax.random.fold_in(key, 3), REPLICAS, INNER, D)


def level_of(rng, shape, cuts, smallest, largest):
    factor_of = 1.0
    for position, parts in cuts:
        heights = jax.random.uniform(jax.random.fold_in(jax.random.fold_in(rng, 6), position), (parts,), jnp.float32, smallest / len(cuts), largest / len(cuts))
        factor_of = factor_of * jnp.repeat(jnp.exp(heights), shape[position] // parts).reshape((-1,) + (1,) * (len(shape) - 1 - position))
    return factor_of


def bell_draw(rng, extent, spread, limit, shards=(), held_as=jnp.bfloat16):
    values = spread * jax.random.normal(rng, extent, jnp.float32)
    if shards:
        values = values * level_of(rng, extent, shards, -0.22, 0.18)
    return jnp.clip(values, -limit, limit).astype(held_as)


def setup_inputs(seed: int = 0) -> dict:
    key_of = jax.random.split(jax.random.key(seed), 13)
    expand_gradient = draw_expand_gradient(jax.random.fold_in(key_of[12], 71), 0)
    expand_master = bell_draw(key_of[1], (D, FF), 0.02, 0.12, ((0, 128), (1, 4)), jnp.float32)
    expand_rows = jnp.clip(jnp.exp(math.log(1.0) - 4.6051702 * jax.random.uniform(key_of[2], (D,), jnp.float32) ** level_of(key_of[2], (D,), ((0, 128),), -0.2, 0.2)), 0.01, 1.0)
    expand_columns = jnp.clip(jnp.exp(math.log(1.0) - 4.6051702 * jax.random.uniform(key_of[3], (FF,), jnp.float32) ** level_of(key_of[3], (FF,), ((0, 4),), -0.2, 0.2)), 0.01, 1.0)
    contract_gradient = draw_contract_gradient(jax.random.fold_in(key_of[12], 71), 0)
    contract_master = bell_draw(key_of[5], (FF, D), 0.02, 0.12, ((0, 128), (1, 4)), jnp.float32)
    contract_rows = jnp.clip(jnp.exp(math.log(1.0) - 4.6051702 * jax.random.uniform(key_of[6], (FF,), jnp.float32) ** level_of(key_of[6], (FF,), ((0, 128),), -0.2, 0.2)), 0.01, 1.0)
    contract_columns = jnp.clip(jnp.exp(math.log(1.0) - 4.6051702 * jax.random.uniform(key_of[7], (D,), jnp.float32) ** level_of(key_of[7], (D,), ((0, 4),), -0.2, 0.2)), 0.01, 1.0)
    attend_gradient = draw_attend_gradient(jax.random.fold_in(key_of[12], 71), 0)
    attend_master = bell_draw(key_of[9], (INNER, D), 0.02, 0.12, ((0, 128), (1, 4)), jnp.float32)
    attend_rows = jnp.clip(jnp.exp(math.log(1.0) - 4.6051702 * jax.random.uniform(key_of[10], (INNER,), jnp.float32) ** level_of(key_of[10], (INNER,), ((0, 128),), -0.2, 0.2)), 0.01, 1.0)
    attend_columns = jnp.clip(jnp.exp(math.log(1.0) - 4.6051702 * jax.random.uniform(key_of[11], (D,), jnp.float32) ** level_of(key_of[11], (D,), ((0, 4),), -0.2, 0.2)), 0.01, 1.0)
    return dict(expand_gradient=expand_gradient, expand_master=expand_master, expand_rows=expand_rows, expand_columns=expand_columns, contract_gradient=contract_gradient, contract_master=contract_master, contract_rows=contract_rows, contract_columns=contract_columns, attend_gradient=attend_gradient, attend_master=attend_master, attend_rows=attend_rows, attend_columns=attend_columns)


def adapt(gradient, master, row_stat, column_stat):
    total = gradient[0].astype(jnp.float32)
    for which in range(1, gradient.shape[0]):
        total = total + gradient[which].astype(jnp.float32)
    mean_grad = total / gradient.shape[0]
    squares = mean_grad * mean_grad + 1e-30
    rows_next = 0.9 * row_stat + 0.1 * lax.optimization_barrier(jnp.mean(squares, axis=1))
    columns_next = 0.9 * column_stat + 0.1 * lax.optimization_barrier(jnp.mean(squares, axis=0))
    row_mean = jnp.mean(rows_next)
    update_raw = mean_grad * jnp.sqrt(row_mean / (rows_next[:, None] * columns_next[None, :]))
    clip_scale = jnp.maximum(1.0, jnp.sqrt(jnp.mean(update_raw * update_raw)))
    step_taken = update_raw / clip_scale
    updated = master - 0.01 * step_taken
    return (updated, updated.astype(jnp.bfloat16), rows_next, columns_next, step_taken)

def reference(expand_gradient, expand_master, expand_rows, expand_columns, contract_gradient, contract_master, contract_rows, contract_columns, attend_gradient, attend_master, attend_rows, attend_columns):
    first = adapt(expand_gradient, expand_master, expand_rows, expand_columns)
    second = adapt(contract_gradient, contract_master, contract_rows, contract_columns)
    third = adapt(attend_gradient, attend_master, attend_rows, attend_columns)
    return (first[0], first[1], first[2], first[3], first[4], second[0], second[1], second[2], second[3], second[4], third[0], third[1], third[2], third[3], third[4])
```

```python
import jax
import jax.numpy as jnp
from jax import lax
from jax.experimental import pallas as pl
from jax.experimental.pallas import tpu as pltpu
from jax.sharding import Mesh
from jax.sharding import PartitionSpec as P

MESH = pl.DeviceIdType.MESH
F32 = jnp.float32
BF16 = jnp.bfloat16

ROW = ("zhi", "x", "core")
ROW_DP = ("zhi", "x", "core", "dp")

tiny_square = 1e-30
decay_rate = 0.9
learn_rate = 0.01

N = 8
HEIGHTS = (32, 40, 32)
WIDTHS = (1280, 1024, 1024)
FULL_ROWS = (4096, 5120, 4096)
FULL_COLS = (5120, 4096, 4096)
BATCHES = ((0, 1), (2,))
LAYOUT = (((0, 0, 0, 8), (1, 1, 0, 8), (2, 0, 8, 10)), ((0, 2, 0, 8),))
Y_ROWS = (0, 32, 72)


def remote(src, dst, send_sem, recv_sem, device):
    return pltpu.make_async_remote_copy(
        src_ref=src, dst_ref=dst, send_sem=send_sem, recv_sem=recv_sem, device_id=device, device_id_type=MESH
    )


def to_column(row, height):
    sub = lax.broadcasted_iota(jnp.int32, (height, 128), 0)
    lane = lax.broadcasted_iota(jnp.int32, (height, 128), 1)
    return jnp.sum(jnp.where(sub == lane, jnp.broadcast_to(row, (height, 128)), 0.0), axis=1, keepdims=True)


def to_row(column, height):
    sub = lax.broadcasted_iota(jnp.int32, (height, 128), 0)
    lane = lax.broadcasted_iota(jnp.int32, (height, 128), 1)
    return jnp.sum(jnp.where(sub == lane, jnp.broadcast_to(column, (height, 128)), 0.0), axis=0, keepdims=True)


def kernel(*refs):
    grads, masters, rows, columns = refs[0:3], refs[3:6], refs[6:9], refs[9:12]
    updated, weights, rows_next, columns_next, steps = refs[12:15], refs[15:18], refs[18:21], refs[21:24], refs[24:27]
    (
        part0, part1, part2, raw0, raw1, raw2, acc0, acc1, acc2,
        rfac0, rfac1, rfac2,
        ysend, yrecv, piece, pieces_in, zsend, zrecv, total, fin, colstat,
        rs_send, rs_recv, ag_send, ag_recv, y_sems, p_sems, z_sems, f_sems,
    ) = refs[27:]
    parts, raws, accs, rfacs = (part0, part1, part2), (raw0, raw1, raw2), (acc0, acc1, acc2), (rfac0, rfac1, rfac2)

    k = lax.axis_index("dp")
    zhi, x, core, y = lax.axis_index("zhi"), lax.axis_index("x"), lax.axis_index("core"), lax.axis_index("col")
    p = x * 2 + core
    q = zhi * 8 + k
    n = y * 8 + p

    def z_peer(o):
        t = lax.rem(q + o, 16)
        return {"zhi": t // 8, "dp": lax.rem(t, 8)}

    def p_peer(t):
        return {"x": t // 2, "core": lax.rem(t, 2)}

    def plane_peer(o):
        t = lax.rem(n + o, 32)
        s = lax.rem(t, 8)
        return {"x": s // 2, "core": lax.rem(s, 2), "col": t // 8}

    barrier = pltpu.get_barrier_semaphore()

    @pl.loop(1, 16)
    def _(o):
        pl.semaphore_signal(barrier, inc=1, device_id=z_peer(o), device_id_type=MESH)

    @pl.loop(1, 32)
    def _(o):
        pl.semaphore_signal(barrier, inc=1, device_id=plane_peer(o), device_id_type=MESH)

    pl.semaphore_wait(barrier, 46)

    a = k // 4
    near = jnp.where(a == 0, k, 7 - k)
    far = 7 - near

    def real(jd, d):
        return jd + d * (7 - 2 * jd)

    def raw_copy(m, d, source, jd):
        j = real(jd, d)
        return remote(
            grads[m].at[j], raws[m].at[d, source, j], rs_send.at[m, d, j], rs_recv.at[m, source, d, j],
            {"dp": real(jnp.minimum(jd, 2), d)},
        )

    def part_copy(m, d, here, jd):
        j = real(jd, d)
        return remote(
            parts[m].at[d, j], parts[m].at[d, j], rs_send.at[m, d, j], rs_recv.at[m, 0, d, j],
            {"dp": real(jnp.minimum(here + 1, 7), d)},
        )

    def send_raw(m):
        @pl.when(near < 2)
        def _():
            @pl.loop(0, 7)
            def _(s):
                jd = 7 - s

                @pl.when(jd > near)
                def _():
                    raw_copy(m, a, near, jd).start()

    def forward_first(m, jd):
        j = real(jd, a)

        @pl.when((near == 2) & (jd > near))
        def _():
            raw_copy(m, a, 0, jd).wait_recv()
            raw_copy(m, a, 1, jd).wait_recv()
            parts[m][a, j] = raws[m][a, 0, j].astype(F32) + raws[m][a, 1, j].astype(F32) + grads[m][j].astype(F32)
            part_copy(m, a, near, jd).start()

        @pl.when((near == 3) & (jd > near))
        def _():
            forward_part(m, a, near, jd)

    def forward_part(m, d, here, jd):
        j = real(jd, d)
        part_copy(m, d, here, jd).wait_recv()
        parts[m][d, j] = parts[m][d, j] + grads[m][j].astype(F32)
        part_copy(m, d, here, jd).start()

    lag = jnp.where(near == 2, 5, jnp.where(near == 3, 2, 0))

    def reduce_chain(m):
        @pl.loop(0, 12)
        def _(u):
            @pl.when(u < 7)
            def _():
                forward_first(m, 7 - u)

            s = u - lag

            @pl.when((s >= 0) & (s < 7) & (7 - s > far))
            def _():
                forward_part(m, 1 - a, far, 7 - s)

    def own_block(m):
        b = 1 - a
        part_copy(m, b, far, far).wait_recv()
        accs[m][...] = parts[m][b, k] + grads[m][k].astype(F32)

        @pl.when((near == 1) | (near == 2))
        def _():
            raw_copy(m, a, 0, near).wait_recv()
            accs[m][...] = accs[m][...] + raws[m][a, 0, k].astype(F32)

        @pl.when(near == 2)
        def _():
            raw_copy(m, a, 1, near).wait_recv()
            accs[m][...] = accs[m][...] + raws[m][a, 1, k].astype(F32)

        @pl.when(near == 3)
        def _():
            part_copy(m, a, near, near).wait_recv()
            accs[m][...] = accs[m][...] + parts[m][a, k]

        accs[m][...] = accs[m][...] * 0.125

    def y_copy(b, o):
        lo = Y_ROWS[BATCHES[b][0]]
        size = sum(HEIGHTS[m] for m in BATCHES[b])
        t = lax.rem(y + o, 4)
        return remote(
            ysend.at[pl.ds(lo, size)], yrecv.at[o, pl.ds(lo, size)], y_sems.at[0, b, o], y_sems.at[1, b, o], {"col": t}
        )

    def stats_rows(b):
        for m in BATCHES[b]:
            square = accs[m][...] * accs[m][...] + tiny_square
            total_row = jnp.sum(square, axis=1, keepdims=True)
            ysend[pl.ds(Y_ROWS[m], HEIGHTS[m])] = jnp.broadcast_to(total_row, (HEIGHTS[m], 128))
        for o in range(1, 4):
            y_copy(b, o).start()

    def p_copy(b, o):
        t = lax.rem(p + o, 8)
        return remote(piece.at[b, t], pieces_in.at[b, o], p_sems.at[0, b, o], p_sems.at[1, b, o], p_peer(t))

    def stats_columns(b):
        for o in range(1, 4):
            y_copy(b, o).wait_recv()
        piece[b] = jnp.zeros((8, 8, 128), F32)
        for m in BATCHES[b]:
            height = HEIGHTS[m]
            at = pl.ds(Y_ROWS[m], height)
            across = (ysend[at] + yrecv[1, at]) + (yrecv[2, at] + yrecv[3, at])
            old = to_column(rows[m][...], height)
            new = decay_rate * old + (1.0 - decay_rate) * (across / FULL_COLS[m])
            rfacs[m][...] = new
            new_column = new[:, 0:1]
            rows_next[m][...] = to_row(new_column, height)
            row_sum = jnp.sum(new, axis=0, keepdims=True)
            g = accs[m][...]
            square = g * g
            plain = jnp.sum(square + tiny_square, axis=0, keepdims=True)
            weighted = jnp.sum(square * (1.0 / new_column), axis=0, keepdims=True)
            for slot, owner, lo, hi in LAYOUT[b]:
                if owner != m:
                    continue
                for group in range(lo, hi):
                    cut = slice(128 * group, 128 * group + 128)
                    piece[b, group - lo, 2 * slot : 2 * slot + 1] = plain[:, cut]
                    piece[b, group - lo, 2 * slot + 1 : 2 * slot + 2] = weighted[:, cut]
            at_row = 7 - BATCHES[b].index(m)
            for which in range(8):
                piece[b, which, at_row : at_row + 1] = row_sum
        for o in range(1, 8):
            p_copy(b, o).start()

    def z_copy(b, o):
        return remote(zsend.at[b], zrecv.at[b, o], z_sems.at[0, b, o], z_sems.at[1, b, o], z_peer(o))

    def stats_depth(b):
        tile = piece[b, p]
        for o in range(1, 8):
            p_copy(b, o).wait_recv()
            tile = tile + pieces_in[b, o]
        zsend[b] = tile

        @pl.loop(1, 16)
        def _(o):
            z_copy(b, o).start()

        colstat[b] = jnp.ones((8, 8, 128), F32)
        for slot, m, lo, hi in LAYOUT[b]:
            for group in range(lo, hi):
                cut = slice(128 * group, 128 * group + 128)
                colstat[b, group - lo, 2 * slot : 2 * slot + 1] = columns[m][:, cut]

    def f_copy(b, o):
        return remote(fin.at[b, n], fin.at[b, n], f_sems.at[0, b, o], f_sems.at[1, b, o], plane_peer(o))

    def next_column(old, total_square, m):
        return decay_rate * old + (1.0 - decay_rate) * (total_square / FULL_ROWS[m])

    def stats_plane(b):
        @pl.loop(1, 16)
        def _(o):
            z_copy(b, o).wait_recv()

        tile = zsend[b]
        for o in range(1, 16):
            tile = tile + zrecv[b, o]
        total[b] = tile
        fin[b, n] = tile
        for slot, m, lo, hi in LAYOUT[b]:
            plain = total[b, 2 * slot : 2 * slot + 1]
            weighted = total[b, 2 * slot + 1 : 2 * slot + 2]
            new = next_column(colstat[b, p, 2 * slot : 2 * slot + 1], plain, m)
            ratio = jnp.sum(weighted / new, axis=1, keepdims=True)
            fin[b, n, 2 * slot + 1 : 2 * slot + 2] = jnp.broadcast_to(ratio, (1, 128))

        @pl.loop(1, 32)
        def _(o):
            f_copy(b, o).start()

    def finish(b):
        @pl.loop(1, 32)
        def _(o):
            f_copy(b, o).wait_recv()

        everyone = fin[b, 0]
        for which in range(1, 32):
            everyone = everyone + fin[b, which]
        for m in BATCHES[b]:
            for slot, owner, lo, hi in LAYOUT[b]:
                if owner != m:
                    continue
                for group in range(lo, hi):
                    cut = slice(128 * group, 128 * group + 128)
                    plain = fin[b, y * 8 + (group - lo), 2 * slot : 2 * slot + 1]
                    columns_next[m][:, cut] = next_column(columns[m][:, cut], plain, m)
            at_row = 7 - BATCHES[b].index(m)
            row_mean = total[b, at_row : at_row + 1] / FULL_ROWS[m]
            ratio = sum(
                everyone[2 * slot + 1 : 2 * slot + 2] for slot, owner, _, _ in LAYOUT[b] if owner == m
            )
            mean_square = row_mean * ratio / (FULL_ROWS[m] * FULL_COLS[m])
            clip = jnp.maximum(1.0, jnp.sqrt(mean_square))
            row_scale = (jnp.sqrt(row_mean) / clip) / jnp.sqrt(rfacs[m][...])
            column_scale = 1.0 / jnp.sqrt(columns_next[m][...])
            step = accs[m][...] * row_scale[:, 0:1] * column_scale
            steps[m][...] = step
            new = masters[m][...] - learn_rate * step
            updated[m][...] = new
            weights[m][k] = new.astype(BF16)

    def w_copy(m, d, i):
        to = jnp.clip(k + 1 - 2 * d, 0, 7)
        return remote(weights[m].at[i], weights[m].at[i], ag_send.at[m, d, i], ag_recv.at[m, i], {"dp": to})

    def gather_start(m):
        for d in (0, 1):

            @pl.when(k != 7 * (1 - d))
            def _():
                w_copy(m, d, k).start()

    def gather_step(m, s):
        for d in (0, 1):
            i = k - s if d == 0 else k + s

            @pl.when((i >= 0) & (i <= 7))
            def _():
                w_copy(m, d, i).wait_recv()

                @pl.when(k != 7 * (1 - d))
                def _():
                    w_copy(m, d, i).start()

    for m in range(3):
        send_raw(m)
    for m in range(3):
        reduce_chain(m)
    for m in range(3):
        own_block(m)
    for b in (0, 1):
        stats_rows(b)
    for b in (0, 1):
        stats_columns(b)
    for b in (0, 1):
        stats_depth(b)
    for b in (0, 1):
        stats_plane(b)
    for b in (0, 1):
        finish(b)
    for m in range(3):
        gather_start(m)

    @pl.loop(1, 8)
    def _(s):
        for m in range(3):
            gather_step(m, s)

    @pl.loop(0, 8)
    def _(j):
        for m in range(3):

            @pl.when((near < 2) & (real(j, a) > near))
            def _():
                raw_copy(m, a, near, real(j, a)).wait_send()

            @pl.when((near >= 2) & (real(j, a) > near))
            def _():
                part_copy(m, a, near, real(j, a)).wait_send()

            @pl.when(real(j, 1 - a) > far)
            def _():
                part_copy(m, 1 - a, far, real(j, 1 - a)).wait_send()

            for d in (0, 1):
                held = (j <= k) if d == 0 else (j >= k)

                @pl.when(held & (k != 7 * (1 - d)))
                def _():
                    w_copy(m, d, j).wait_send()

    for b in (0, 1):
        for o in range(1, 4):
            y_copy(b, o).wait_send()
        for o in range(1, 8):
            p_copy(b, o).wait_send()

        @pl.loop(1, 16)
        def _(o):
            z_copy(b, o).wait_send()

        @pl.loop(1, 32)
        def _(o):
            f_copy(b, o).wait_send()


def body(*args):
    grads = [args[4 * m].reshape(N, HEIGHTS[m], WIDTHS[m]) for m in range(3)]
    masters = [args[4 * m + 1] for m in range(3)]
    rows = [jnp.pad(args[4 * m + 2], (0, 128 - HEIGHTS[m])).reshape(1, 128) for m in range(3)]
    columns = [args[4 * m + 3].reshape(1, WIDTHS[m]) for m in range(3)]
    shape = jax.ShapeDtypeStruct
    blocks = list(zip(HEIGHTS, WIDTHS))
    out_shape = (
        [shape(b, F32) for b in blocks]
        + [shape((N, *b), BF16) for b in blocks]
        + [shape((1, 128), F32)] * 3
        + [shape((1, w), F32) for w in WIDTHS]
        + [shape(b, F32) for b in blocks]
    )
    vmem = pl.BlockSpec(memory_space=pltpu.VMEM)
    dma = pltpu.SemaphoreType.DMA
    out = pl.pallas_call(
        kernel,
        out_shape=out_shape,
        in_specs=[vmem] * 12,
        out_specs=[vmem] * 15,
        scratch_shapes=(
            [pltpu.VMEM((2, N, *b), F32) for b in blocks]
            + [pltpu.VMEM((2, 2, N, *b), BF16) for b in blocks]
            + [pltpu.VMEM(b, F32) for b in blocks]
            + [pltpu.VMEM((h, 128), F32) for h in HEIGHTS]
            + [
                pltpu.VMEM((104, 128), F32),
                pltpu.VMEM((4, 104, 128), F32),
                pltpu.VMEM((2, 8, 8, 128), F32),
                pltpu.VMEM((2, 8, 8, 128), F32),
                pltpu.VMEM((2, 8, 128), F32),
                pltpu.VMEM((2, 16, 8, 128), F32),
                pltpu.VMEM((2, 8, 128), F32),
                pltpu.VMEM((2, 32, 8, 128), F32),
                pltpu.VMEM((2, 8, 8, 128), F32),
                dma((3, 2, 8)),
                dma((3, 2, 2, 8)),
                dma((3, 2, 8)),
                dma((3, 8)),
                dma((2, 2, 4)),
                dma((2, 2, 8)),
                dma((2, 2, 16)),
                dma((2, 2, 32)),
            ]
        ),
        compiler_params=pltpu.CompilerParams(
            collective_id=0, has_side_effects=True, vmem_limit_bytes=60 * 1024 * 1024
        ),
    )(*grads, *masters, *rows, *columns)
    result = []
    for m in range(3):
        result += [
            out[m],
            out[3 + m].reshape(N * HEIGHTS[m], WIDTHS[m]),
            out[6 + m][0, : HEIGHTS[m]],
            out[9 + m].reshape(WIDTHS[m]),
            out[12 + m],
        ]
    return tuple(result)


def solution(mesh):
    finer = Mesh(mesh.devices.reshape(mesh.shape["dp"], 2, 4, 2, mesh.shape["col"]), ("dp", *ROW, "col"))
    one = (P("dp", ROW, "col"), P(ROW_DP, "col"), P(ROW_DP), P("col"))
    back = (P(ROW_DP, "col"), P(ROW, "col"), P(ROW_DP), P("col"), P(ROW_DP, "col"))
    return jax.shard_map(body, mesh=finer, in_specs=one * 3, out_specs=back * 3, check_vma=False)
```

```python
import jax
import jax.numpy as jnp
from jax import lax
from jax.experimental import pallas as pl
from jax.experimental.pallas import tpu as pltpu
from jax.sharding import Mesh
from jax.sharding import PartitionSpec as P

MESH = pl.DeviceIdType.MESH
F32 = jnp.float32
BF16 = jnp.bfloat16

ROW = ("zhi", "x", "core")
ROW_DP = ("zhi", "x", "core", "dp")

tiny_square = 1e-30
decay_rate = 0.9
learn_rate = 0.01

N = 8
HEIGHTS = (32, 40, 32)
WIDTHS = (1280, 1024, 1024)
FULL_ROWS = (4096, 5120, 4096)
FULL_COLS = (5120, 4096, 4096)
BATCHES = ((0,), (1, 2))
LAYOUT = (((0, 0, 0, 8), (1, 0, 8, 10)), ((0, 1, 0, 8), (1, 2, 0, 8)))


def remote(src, dst, send_sem, recv_sem, device):
    return pltpu.make_async_remote_copy(
        src_ref=src, dst_ref=dst, send_sem=send_sem, recv_sem=recv_sem, device_id=device, device_id_type=MESH
    )


def to_column(row, height):
    sub = lax.broadcasted_iota(jnp.int32, (height, 128), 0)
    lane = lax.broadcasted_iota(jnp.int32, (height, 128), 1)
    return jnp.sum(jnp.where(sub == lane, jnp.broadcast_to(row, (height, 128)), 0.0), axis=1, keepdims=True)


def to_row(column, height):
    sub = lax.broadcasted_iota(jnp.int32, (height, 128), 0)
    lane = lax.broadcasted_iota(jnp.int32, (height, 128), 1)
    return jnp.sum(jnp.where(sub == lane, jnp.broadcast_to(column, (height, 128)), 0.0), axis=0, keepdims=True)


def kernel(*refs):
    grads, masters, rows, columns = refs[0:3], refs[3:6], refs[6:9], refs[9:12]
    updated, weights, rows_next, columns_next, steps = refs[12:15], refs[15:18], refs[18:21], refs[21:24], refs[24:27]
    (
        part0, part1, part2, raw0, raw1, raw2, acc0, acc1, acc2,
        rfac0, rfac1, rfac2,
        ysend, yrecv, piece, pieces_in, zsend, zrecv, total, fin, colstat,
        rs_send, rs_recv, ag_send, ag_recv, y_sems, p_sems, z_sems, f_sems,
    ) = refs[27:]
    parts, raws, accs, rfacs = (part0, part1, part2), (raw0, raw1, raw2), (acc0, acc1, acc2), (rfac0, rfac1, rfac2)

    k = lax.axis_index("dp")
    zhi, x, core, y = lax.axis_index("zhi"), lax.axis_index("x"), lax.axis_index("core"), lax.axis_index("col")
    p = x * 2 + core
    q = zhi * 8 + k
    n = y * 8 + p

    def z_peer(o):
        t = lax.rem(q + o, 16)
        return {"zhi": t // 8, "dp": lax.rem(t, 8)}

    def p_peer(t):
        return {"x": t // 2, "core": lax.rem(t, 2)}

    def plane_peer(o):
        t = lax.rem(n + o, 32)
        s = lax.rem(t, 8)
        return {"x": s // 2, "core": lax.rem(s, 2), "col": t // 8}

    barrier = pltpu.get_barrier_semaphore()

    @pl.loop(1, 16)
    def _(o):
        pl.semaphore_signal(barrier, inc=1, device_id=z_peer(o), device_id_type=MESH)

    @pl.loop(1, 32)
    def _(o):
        pl.semaphore_signal(barrier, inc=1, device_id=plane_peer(o), device_id_type=MESH)

    pl.semaphore_wait(barrier, 46)

    a = k // 4
    near = jnp.where(a == 0, k, 7 - k)
    far = 7 - near

    def real(jd, d):
        return jd + d * (7 - 2 * jd)

    def half(m, c):
        return pl.ds(c * (WIDTHS[m] // 2), WIDTHS[m] // 2)

    def raw_copy(m, jd, c):
        j = real(jd, a)
        return remote(
            grads[m].at[j, :, half(m, c)], raws[m].at[a, j, :, half(m, c)], rs_send.at[m, a, j, c],
            rs_recv.at[m, a, j, c], {"dp": real(1, a)},
        )

    def part_copy(m, d, here, jd, c):
        j = real(jd, d)
        block = parts[m].at[d, j, :, half(m, c)]
        return remote(
            block, block, rs_send.at[m, d, j, c], rs_recv.at[m, d, j, c], {"dp": real(jnp.minimum(here + 1, 7), d)}
        )

    def send_raw(m):
        @pl.when(near == 0)
        def _():
            @pl.loop(0, 7)
            def _(s):
                for c in (0, 1):
                    raw_copy(m, 7 - s, c).start()

    def forward_first(m, jd):
        j = real(jd, a)

        @pl.when((near == 1) & (jd > near))
        def _():
            for c in (0, 1):
                cut = half(m, c)
                raw_copy(m, jd, c).wait_recv()
                parts[m][a, j, :, cut] = raws[m][a, j, :, cut].astype(F32) + grads[m][j, :, cut].astype(F32)
                part_copy(m, a, near, jd, c).start()

        @pl.when((near >= 2) & (jd > near))
        def _():
            forward_part(m, a, near, jd)

    def forward_part(m, d, here, jd):
        j = real(jd, d)
        for c in (0, 1):
            cut = half(m, c)
            part_copy(m, d, here, jd, c).wait_recv()
            parts[m][d, j, :, cut] = parts[m][d, j, :, cut] + grads[m][j, :, cut].astype(F32)
            part_copy(m, d, here, jd, c).start()

    def forward_second(m, r):
        @pl.when((r >= 0) & (7 - r > far))
        def _():
            forward_part(m, 1 - a, far, 7 - r)

    def own_block(m):
        b = 1 - a
        for c in (0, 1):
            part_copy(m, b, far, far, c).wait_recv()
        accs[m][...] = parts[m][b, k] + grads[m][k].astype(F32)

        @pl.when(near == 1)
        def _():
            for c in (0, 1):
                raw_copy(m, near, c).wait_recv()
            accs[m][...] = accs[m][...] + raws[m][a, k].astype(F32)

        @pl.when(near >= 2)
        def _():
            for c in (0, 1):
                part_copy(m, a, near, near, c).wait_recv()
            accs[m][...] = accs[m][...] + parts[m][a, k]

        accs[m][...] = accs[m][...] * 0.125

    def y_copy(b, o):
        t = lax.rem(y + o, 4)
        return remote(ysend.at[b], yrecv.at[b, o], y_sems.at[0, b, o], y_sems.at[1, b, o], {"col": t})

    def stats_rows(b):
        for at_row, m in enumerate(BATCHES[b]):
            square = accs[m][...] * accs[m][...] + tiny_square
            total_row = jnp.sum(square, axis=1, keepdims=True)
            ysend[b, at_row : at_row + 1] = to_row(total_row, HEIGHTS[m])
        for o in range(1, 4):
            y_copy(b, o).start()

    def p_copy(b, o):
        t = lax.rem(p + o, 8)
        return remote(piece.at[b, t], pieces_in.at[b, o], p_sems.at[0, b, o], p_sems.at[1, b, o], p_peer(t))

    def stats_columns(b):
        for o in range(1, 4):
            y_copy(b, o).wait_recv()
        piece[b] = jnp.zeros((8, 8, 128), F32)
        for m in BATCHES[b]:
            height = HEIGHTS[m]
            at = slice(BATCHES[b].index(m), BATCHES[b].index(m) + 1)
            across = (ysend[b, at] + yrecv[b, 1, at]) + (yrecv[b, 2, at] + yrecv[b, 3, at])
            new = decay_rate * rows[m][...] + (1.0 - decay_rate) * (across / FULL_COLS[m])
            rows_next[m][...] = new
            new_column = to_column(new, height)
            rfacs[m][...] = jnp.broadcast_to(new_column, (height, 128))
            row_sum = jnp.broadcast_to(jnp.sum(new_column, axis=0, keepdims=True), (1, 128))
            g = accs[m][...]
            square = g * g
            plain = jnp.sum(square + tiny_square, axis=0, keepdims=True)
            weighted = jnp.sum(square * (1.0 / new_column), axis=0, keepdims=True)
            for slot, owner, lo, hi in LAYOUT[b]:
                if owner != m:
                    continue
                for group in range(lo, hi):
                    cut = slice(128 * group, 128 * group + 128)
                    piece[b, group - lo, 2 * slot : 2 * slot + 1] = plain[:, cut]
                    piece[b, group - lo, 2 * slot + 1 : 2 * slot + 2] = weighted[:, cut]
            at_row = 7 - BATCHES[b].index(m)
            for which in range(8):
                piece[b, which, at_row : at_row + 1] = row_sum
        for o in range(1, 8):
            p_copy(b, o).start()

    def z_copy(b, o):
        return remote(zsend.at[b], zrecv.at[b, o], z_sems.at[0, b, o], z_sems.at[1, b, o], z_peer(o))

    def stats_depth(b):
        tile = piece[b, p]
        for o in range(1, 8):
            p_copy(b, o).wait_recv()
            tile = tile + pieces_in[b, o]
        zsend[b] = tile

        @pl.loop(1, 16)
        def _(o):
            z_copy(b, o).start()

        colstat[b] = jnp.ones((8, 8, 128), F32)
        for slot, m, lo, hi in LAYOUT[b]:
            for group in range(lo, hi):
                cut = slice(128 * group, 128 * group + 128)
                colstat[b, group - lo, 2 * slot : 2 * slot + 1] = columns[m][:, cut]

    def f_copy(b, o):
        return remote(fin.at[b, n], fin.at[b, n], f_sems.at[0, b, o], f_sems.at[1, b, o], plane_peer(o))

    def next_column(old, total_square, m):
        return decay_rate * old + (1.0 - decay_rate) * (total_square / FULL_ROWS[m])

    def stats_plane(b):
        @pl.loop(1, 16)
        def _(o):
            z_copy(b, o).wait_recv()

        tile = zsend[b]
        for o in range(1, 16):
            tile = tile + zrecv[b, o]
        total[b] = tile
        fin[b, n] = tile
        for slot, m, lo, hi in LAYOUT[b]:
            plain = total[b, 2 * slot : 2 * slot + 1]
            weighted = total[b, 2 * slot + 1 : 2 * slot + 2]
            new = next_column(colstat[b, p, 2 * slot : 2 * slot + 1], plain, m)
            ratio = jnp.sum(weighted / new, axis=1, keepdims=True)
            fin[b, n, 2 * slot + 1 : 2 * slot + 2] = jnp.broadcast_to(ratio, (1, 128))

        @pl.loop(1, 32)
        def _(o):
            f_copy(b, o).start()

    def finish(b):
        @pl.loop(1, 32)
        def _(o):
            f_copy(b, o).wait_recv()

        everyone = fin[b, 0]
        for which in range(1, 32):
            everyone = everyone + fin[b, which]
        for m in BATCHES[b]:
            for slot, owner, lo, hi in LAYOUT[b]:
                if owner != m:
                    continue
                for group in range(lo, hi):
                    cut = slice(128 * group, 128 * group + 128)
                    plain = fin[b, y * 8 + (group - lo), 2 * slot : 2 * slot + 1]
                    columns_next[m][:, cut] = next_column(columns[m][:, cut], plain, m)
            at_row = 7 - BATCHES[b].index(m)
            row_mean = total[b, at_row : at_row + 1] / FULL_ROWS[m]
            ratio = sum(
                everyone[2 * slot + 1 : 2 * slot + 2] for slot, owner, _, _ in LAYOUT[b] if owner == m
            )
            mean_square = row_mean * ratio / (FULL_ROWS[m] * FULL_COLS[m])
            clip = jnp.maximum(1.0, jnp.sqrt(mean_square))
            row_scale = (jnp.sqrt(row_mean) / clip) / jnp.sqrt(rfacs[m][...])
            column_scale = 1.0 / jnp.sqrt(columns_next[m][...])
            step = accs[m][...] * row_scale[:, 0:1] * column_scale
            steps[m][...] = step
            new = masters[m][...] - learn_rate * step
            updated[m][...] = new
            weights[m][k] = new.astype(BF16)

    def w_copy(m, d, i):
        to = jnp.clip(k + 1 - 2 * d, 0, 7)
        return remote(weights[m].at[i], weights[m].at[i], ag_send.at[m, d, i], ag_recv.at[m, i], {"dp": to})

    def gather_start(m):
        for d in (0, 1):

            @pl.when(k != 7 * (1 - d))
            def _():
                w_copy(m, d, k).start()

    def gather_step(m, s):
        for d in (0, 1):
            i = k - s if d == 0 else k + s

            @pl.when((i >= 0) & (i <= 7))
            def _():
                w_copy(m, d, i).wait_recv()

                @pl.when(k != 7 * (1 - d))
                def _():
                    w_copy(m, d, i).start()

    for m in range(3):
        send_raw(m)

    lag = jnp.where(near == 1, 6, jnp.where(near == 2, 4, 2))
    lag_pair = jnp.where(near == 1, 4, jnp.where(near == 2, 2, 1))

    @pl.loop(0, 7)
    def _(u):
        forward_first(0, 7 - u)
        forward_second(0, u - lag)

    @pl.loop(0, 7)
    def _(u):
        for m in (1, 2):
            forward_first(m, 7 - u)
        for m in (1, 2):
            forward_second(m, u - lag_pair)

        @pl.when(u == 0)
        def _():
            own_block(0)
            stats_rows(0)

        @pl.when(u == 1)
        def _():
            stats_columns(0)

        @pl.when(u == 2)
        def _():
            stats_depth(0)

        @pl.when(u == 5)
        def _():
            stats_plane(0)

    for m in (1, 2):
        own_block(m)
    stats_rows(1)
    finish(0)
    gather_start(0)
    stats_columns(1)
    gather_step(0, 1)
    stats_depth(1)
    gather_step(0, 2)
    gather_step(0, 3)
    stats_plane(1)
    gather_step(0, 4)
    finish(1)
    for m in (1, 2):
        gather_start(m)
    gather_step(0, 5)
    for m in (1, 2):
        gather_step(m, 1)
    gather_step(0, 6)
    for m in (1, 2):
        gather_step(m, 2)
    gather_step(0, 7)

    @pl.loop(3, 8)
    def _(s):
        for m in (1, 2):
            gather_step(m, s)

    @pl.loop(0, 8)
    def _(j):
        for m in range(3):

            @pl.when((near == 0) & (real(j, a) > 0))
            def _():
                for c in (0, 1):
                    raw_copy(m, real(j, a), c).wait_send()

            @pl.when((near >= 1) & (real(j, a) > near))
            def _():
                for c in (0, 1):
                    part_copy(m, a, near, real(j, a), c).wait_send()

            @pl.when(real(j, 1 - a) > far)
            def _():
                for c in (0, 1):
                    part_copy(m, 1 - a, far, real(j, 1 - a), c).wait_send()

            for d in (0, 1):
                held = (j <= k) if d == 0 else (j >= k)

                @pl.when(held & (k != 7 * (1 - d)))
                def _():
                    w_copy(m, d, j).wait_send()

    for b in (0, 1):
        for o in range(1, 4):
            y_copy(b, o).wait_send()
        for o in range(1, 8):
            p_copy(b, o).wait_send()

        @pl.loop(1, 16)
        def _(o):
            z_copy(b, o).wait_send()

        @pl.loop(1, 32)
        def _(o):
            f_copy(b, o).wait_send()


def body(*args):
    grads = [args[4 * m].reshape(N, HEIGHTS[m], WIDTHS[m]) for m in range(3)]
    masters = [args[4 * m + 1] for m in range(3)]
    rows = [jnp.pad(args[4 * m + 2], (0, 128 - HEIGHTS[m])).reshape(1, 128) for m in range(3)]
    columns = [args[4 * m + 3].reshape(1, WIDTHS[m]) for m in range(3)]
    shape = jax.ShapeDtypeStruct
    blocks = list(zip(HEIGHTS, WIDTHS))
    out_shape = (
        [shape(b, F32) for b in blocks]
        + [shape((N, *b), BF16) for b in blocks]
        + [shape((1, 128), F32)] * 3
        + [shape((1, w), F32) for w in WIDTHS]
        + [shape(b, F32) for b in blocks]
    )
    vmem = pl.BlockSpec(memory_space=pltpu.VMEM)
    dma = pltpu.SemaphoreType.DMA
    out = pl.pallas_call(
        kernel,
        out_shape=out_shape,
        in_specs=[vmem] * 12,
        out_specs=[vmem] * 15,
        scratch_shapes=(
            [pltpu.VMEM((2, N, *b), F32) for b in blocks]
            + [pltpu.VMEM((2, N, *b), BF16) for b in blocks]
            + [pltpu.VMEM(b, F32) for b in blocks]
            + [pltpu.VMEM((h, 128), F32) for h in HEIGHTS]
            + [
                pltpu.VMEM((2, 8, 128), F32),
                pltpu.VMEM((2, 4, 8, 128), F32),
                pltpu.VMEM((2, 8, 8, 128), F32),
                pltpu.VMEM((2, 8, 8, 128), F32),
                pltpu.VMEM((2, 8, 128), F32),
                pltpu.VMEM((2, 16, 8, 128), F32),
                pltpu.VMEM((2, 8, 128), F32),
                pltpu.VMEM((2, 32, 8, 128), F32),
                pltpu.VMEM((2, 8, 8, 128), F32),
                dma((3, 2, 8, 2)),
                dma((3, 2, 8, 2)),
                dma((3, 2, 8)),
                dma((3, 8)),
                dma((2, 2, 4)),
                dma((2, 2, 8)),
                dma((2, 2, 16)),
                dma((2, 2, 32)),
            ]
        ),
        compiler_params=pltpu.CompilerParams(
            collective_id=0, has_side_effects=True, vmem_limit_bytes=60 * 1024 * 1024
        ),
    )(*grads, *masters, *rows, *columns)
    result = []
    for m in range(3):
        result += [
            out[m],
            out[3 + m].reshape(N * HEIGHTS[m], WIDTHS[m]),
            out[6 + m][0, : HEIGHTS[m]],
            out[9 + m].reshape(WIDTHS[m]),
            out[12 + m],
        ]
    return tuple(result)


def solution(mesh):
    finer = Mesh(mesh.devices.reshape(mesh.shape["dp"], 2, 4, 2, mesh.shape["col"]), ("dp", *ROW, "col"))
    one = (P("dp", ROW, "col"), P(ROW_DP, "col"), P(ROW_DP), P("col"))
    back = (P(ROW_DP, "col"), P(ROW, "col"), P(ROW_DP), P("col"), P(ROW_DP, "col"))
    return jax.shard_map(body, mesh=finer, in_specs=one * 3, out_specs=back * 3, check_vma=False)
```

```python
import jax
import jax.numpy as jnp
from jax import lax
from jax.experimental import pallas as pl
from jax.experimental.pallas import tpu as pltpu
from jax.sharding import Mesh
from jax.sharding import PartitionSpec as P

MESH = pl.DeviceIdType.MESH
F32 = jnp.float32
BF16 = jnp.bfloat16

ROW = ("zhi", "x", "core")
ROW_DP = ("zhi", "x", "core", "dp")

tiny_square = 1e-30
decay_rate = 0.9
learn_rate = 0.01

N = 8
HEIGHTS = (32, 40, 32)
WIDTHS = (1280, 1024, 1024)
FULL_ROWS = (4096, 5120, 4096)
FULL_COLS = (5120, 4096, 4096)
BATCHES = ((0,), (1, 2))
LAYOUT = (((0, 0, 0, 8), (1, 0, 8, 10)), ((0, 1, 0, 8), (1, 2, 0, 8)))


def remote(src, dst, send_sem, recv_sem, device):
    return pltpu.make_async_remote_copy(
        src_ref=src, dst_ref=dst, send_sem=send_sem, recv_sem=recv_sem, device_id=device, device_id_type=MESH
    )


def to_column(row, height):
    sub = lax.broadcasted_iota(jnp.int32, (height, 128), 0)
    lane = lax.broadcasted_iota(jnp.int32, (height, 128), 1)
    return jnp.sum(jnp.where(sub == lane, jnp.broadcast_to(row, (height, 128)), 0.0), axis=1, keepdims=True)


def to_row(column, height):
    sub = lax.broadcasted_iota(jnp.int32, (height, 128), 0)
    lane = lax.broadcasted_iota(jnp.int32, (height, 128), 1)
    return jnp.sum(jnp.where(sub == lane, jnp.broadcast_to(column, (height, 128)), 0.0), axis=0, keepdims=True)


def as_row(ref, height):
    return jnp.pad(ref[...].reshape(1, height), ((0, 0), (0, 128 - height)))


def kernel(*refs):
    given = refs[0:12]
    updated, weights, rows_next, columns_next, steps = refs[12:15], refs[15:18], refs[18:21], refs[21:24], refs[24:27]
    (
        part0, part1, part2, raw0, raw1, raw2, acc0, acc1, acc2,
        rfac0, rfac1, rfac2,
        ysend, yrecv, piece, pieces_in, zsend, zrecv, total, fin, colstat,
        rs_send, rs_recv, ag_send, ag_recv, y_sems, p_sems, z_sems, f_sems,
        *held, load_sems,
    ) = refs[27:]
    grads, masters, rows, columns = held[0:3], held[3:6], held[6:9], held[9:12]
    loads = [pltpu.make_async_copy(given[i], held[i], load_sems.at[i]) for i in range(12)]
    for load in loads:
        load.start()
    parts, raws, accs, rfacs = (part0, part1, part2), (raw0, raw1, raw2), (acc0, acc1, acc2), (rfac0, rfac1, rfac2)

    k = lax.axis_index("dp")
    zhi, x, core, y = lax.axis_index("zhi"), lax.axis_index("x"), lax.axis_index("core"), lax.axis_index("col")
    p = x * 2 + core
    q = zhi * 8 + k
    n = y * 8 + p

    def z_peer(o):
        t = lax.rem(q + o, 16)
        return {"zhi": t // 8, "dp": lax.rem(t, 8)}

    def p_peer(t):
        return {"x": t // 2, "core": lax.rem(t, 2)}

    def plane_peer(o):
        t = lax.rem(n + o, 32)
        s = lax.rem(t, 8)
        return {"x": s // 2, "core": lax.rem(s, 2), "col": t // 8}

    barrier = pltpu.get_barrier_semaphore()

    @pl.loop(1, 16)
    def _(o):
        pl.semaphore_signal(barrier, inc=1, device_id=z_peer(o), device_id_type=MESH)

    @pl.loop(1, 32)
    def _(o):
        pl.semaphore_signal(barrier, inc=1, device_id=plane_peer(o), device_id_type=MESH)

    for load in loads:
        load.wait()
    pl.semaphore_wait(barrier, 46)

    a = k // 4
    near = jnp.where(a == 0, k, 7 - k)
    far = 7 - near

    def real(jd, d):
        return jd + d * (7 - 2 * jd)

    def half(m, c):
        return pl.ds(c * (WIDTHS[m] // 2), WIDTHS[m] // 2)

    def raw_copy(m, jd, c):
        j = real(jd, a)
        return remote(
            grads[m].at[j, :, half(m, c)], raws[m].at[a, j, :, half(m, c)], rs_send.at[m, a, j, c],
            rs_recv.at[m, a, j, c], {"dp": real(1, a)},
        )

    def part_copy(m, d, here, jd, c):
        j = real(jd, d)
        block = parts[m].at[d, j, :, half(m, c)]
        return remote(
            block, block, rs_send.at[m, d, j, c], rs_recv.at[m, d, j, c], {"dp": real(jnp.minimum(here + 1, 7), d)}
        )

    def send_raw(m):
        @pl.when(near == 0)
        def _():
            @pl.loop(0, 7)
            def _(s):
                for c in (0, 1):
                    raw_copy(m, 7 - s, c).start()

    def forward_first(m, jd):
        j = real(jd, a)

        @pl.when((near == 1) & (jd > near))
        def _():
            for c in (0, 1):
                cut = half(m, c)
                raw_copy(m, jd, c).wait_recv()
                parts[m][a, j, :, cut] = raws[m][a, j, :, cut].astype(F32) + grads[m][j, :, cut].astype(F32)
                part_copy(m, a, near, jd, c).start()

        @pl.when((near >= 2) & (jd > near))
        def _():
            forward_part(m, a, near, jd)

    def forward_part(m, d, here, jd):
        j = real(jd, d)
        for c in (0, 1):
            cut = half(m, c)
            part_copy(m, d, here, jd, c).wait_recv()
            parts[m][d, j, :, cut] = parts[m][d, j, :, cut] + grads[m][j, :, cut].astype(F32)
            part_copy(m, d, here, jd, c).start()

    def forward_second(m, r):
        @pl.when((r >= 0) & (7 - r > far))
        def _():
            forward_part(m, 1 - a, far, 7 - r)

    def own_block(m):
        b = 1 - a
        for c in (0, 1):
            part_copy(m, b, far, far, c).wait_recv()
        accs[m][...] = parts[m][b, k] + grads[m][k].astype(F32)

        @pl.when(near == 1)
        def _():
            for c in (0, 1):
                raw_copy(m, near, c).wait_recv()
            accs[m][...] = accs[m][...] + raws[m][a, k].astype(F32)

        @pl.when(near >= 2)
        def _():
            for c in (0, 1):
                part_copy(m, a, near, near, c).wait_recv()
            accs[m][...] = accs[m][...] + parts[m][a, k]

        accs[m][...] = accs[m][...] * 0.125

    def y_copy(b, o):
        t = lax.rem(y + o, 4)
        return remote(ysend.at[b], yrecv.at[b, o], y_sems.at[0, b, o], y_sems.at[1, b, o], {"col": t})

    def stats_rows(b):
        for at_row, m in enumerate(BATCHES[b]):
            square = accs[m][...] * accs[m][...] + tiny_square
            total_row = jnp.sum(square, axis=1, keepdims=True)
            ysend[b, at_row : at_row + 1] = to_row(total_row, HEIGHTS[m])
        for o in range(1, 4):
            y_copy(b, o).start()

    def p_copy(b, o):
        t = lax.rem(p + o, 8)
        return remote(piece.at[b, t], pieces_in.at[b, o], p_sems.at[0, b, o], p_sems.at[1, b, o], p_peer(t))

    def stats_columns(b):
        for o in range(1, 4):
            y_copy(b, o).wait_recv()
        piece[b] = jnp.zeros((8, 8, 128), F32)
        for m in BATCHES[b]:
            height = HEIGHTS[m]
            at = slice(BATCHES[b].index(m), BATCHES[b].index(m) + 1)
            across = (ysend[b, at] + yrecv[b, 1, at]) + (yrecv[b, 2, at] + yrecv[b, 3, at])
            new = decay_rate * as_row(rows[m], height) + (1.0 - decay_rate) * (across / FULL_COLS[m])
            rows_next[m][...] = new
            new_column = to_column(new, height)
            rfacs[m][...] = jnp.broadcast_to(new_column, (height, 128))
            row_sum = jnp.broadcast_to(jnp.sum(new_column, axis=0, keepdims=True), (1, 128))
            g = accs[m][...]
            square = g * g
            plain = jnp.sum(square + tiny_square, axis=0, keepdims=True)
            weighted = jnp.sum(square * (1.0 / new_column), axis=0, keepdims=True)
            for slot, owner, lo, hi in LAYOUT[b]:
                if owner != m:
                    continue
                for group in range(lo, hi):
                    cut = slice(128 * group, 128 * group + 128)
                    piece[b, group - lo, 2 * slot : 2 * slot + 1] = plain[:, cut]
                    piece[b, group - lo, 2 * slot + 1 : 2 * slot + 2] = weighted[:, cut]
            at_row = 7 - BATCHES[b].index(m)
            for which in range(8):
                piece[b, which, at_row : at_row + 1] = row_sum
        for o in range(1, 8):
            p_copy(b, o).start()

    def z_copy(b, o):
        return remote(zsend.at[b], zrecv.at[b, o], z_sems.at[0, b, o], z_sems.at[1, b, o], z_peer(o))

    def stats_depth(b):
        tile = piece[b, p]
        for o in range(1, 8):
            p_copy(b, o).wait_recv()
            tile = tile + pieces_in[b, o]
        zsend[b] = tile

        @pl.loop(1, 16)
        def _(o):
            z_copy(b, o).start()

        colstat[b] = jnp.ones((8, 8, 128), F32)
        for slot, m, lo, hi in LAYOUT[b]:
            for group in range(lo, hi):
                cut = slice(128 * group, 128 * group + 128)
                colstat[b, group - lo, 2 * slot : 2 * slot + 1] = columns[m][cut].reshape(1, 128)

    def f_copy(b, o):
        return remote(fin.at[b, n], fin.at[b, n], f_sems.at[0, b, o], f_sems.at[1, b, o], plane_peer(o))

    def next_column(old, total_square, m):
        return decay_rate * old + (1.0 - decay_rate) * (total_square / FULL_ROWS[m])

    def stats_plane(b):
        @pl.loop(1, 16)
        def _(o):
            z_copy(b, o).wait_recv()

        tile = zsend[b]
        for o in range(1, 16):
            tile = tile + zrecv[b, o]
        total[b] = tile
        fin[b, n] = tile
        for slot, m, lo, hi in LAYOUT[b]:
            plain = total[b, 2 * slot : 2 * slot + 1]
            weighted = total[b, 2 * slot + 1 : 2 * slot + 2]
            new = next_column(colstat[b, p, 2 * slot : 2 * slot + 1], plain, m)
            ratio = jnp.sum(weighted / new, axis=1, keepdims=True)
            fin[b, n, 2 * slot + 1 : 2 * slot + 2] = jnp.broadcast_to(ratio, (1, 128))

        @pl.loop(1, 32)
        def _(o):
            f_copy(b, o).start()

    def finish(b):
        @pl.loop(1, 32)
        def _(o):
            f_copy(b, o).wait_recv()

        everyone = fin[b, 0]
        for which in range(1, 32):
            everyone = everyone + fin[b, which]
        for m in BATCHES[b]:
            for slot, owner, lo, hi in LAYOUT[b]:
                if owner != m:
                    continue
                for group in range(lo, hi):
                    cut = slice(128 * group, 128 * group + 128)
                    plain = fin[b, y * 8 + (group - lo), 2 * slot : 2 * slot + 1]
                    columns_next[m][:, cut] = next_column(columns[m][cut].reshape(1, 128), plain, m)
            at_row = 7 - BATCHES[b].index(m)
            row_mean = total[b, at_row : at_row + 1] / FULL_ROWS[m]
            ratio = sum(
                everyone[2 * slot + 1 : 2 * slot + 2] for slot, owner, _, _ in LAYOUT[b] if owner == m
            )
            mean_square = row_mean * ratio / (FULL_ROWS[m] * FULL_COLS[m])
            clip = jnp.maximum(1.0, jnp.sqrt(mean_square))
            row_scale = (jnp.sqrt(row_mean) / clip) / jnp.sqrt(rfacs[m][...])
            column_scale = 1.0 / jnp.sqrt(columns_next[m][...])
            step = accs[m][...] * row_scale[:, 0:1] * column_scale
            steps[m][...] = step
            new = masters[m][...] - learn_rate * step
            updated[m][...] = new
            weights[m][k] = new.astype(BF16)

    def w_copy(m, d, i):
        to = jnp.clip(k + 1 - 2 * d, 0, 7)
        return remote(weights[m].at[i], weights[m].at[i], ag_send.at[m, d, i], ag_recv.at[m, i], {"dp": to})

    def gather_start(m):
        for d in (0, 1):

            @pl.when(k != 7 * (1 - d))
            def _():
                w_copy(m, d, k).start()

    def gather_step(m, s):
        for d in (0, 1):
            i = k - s if d == 0 else k + s

            @pl.when((i >= 0) & (i <= 7))
            def _():
                w_copy(m, d, i).wait_recv()

                @pl.when(k != 7 * (1 - d))
                def _():
                    w_copy(m, d, i).start()

    for m in range(3):
        send_raw(m)

    lag = jnp.where(near == 1, 6, jnp.where(near == 2, 4, 2))
    lag_pair = jnp.where(near == 1, 4, jnp.where(near == 2, 2, 1))

    @pl.loop(0, 7)
    def _(u):
        forward_first(0, 7 - u)
        forward_second(0, u - lag)

    @pl.loop(0, 7)
    def _(u):
        for m in (1, 2):
            forward_first(m, 7 - u)
        for m in (1, 2):
            forward_second(m, u - lag_pair)

        @pl.when(u == 0)
        def _():
            own_block(0)
            stats_rows(0)

        @pl.when(u == 1)
        def _():
            stats_columns(0)

        @pl.when(u == 2)
        def _():
            stats_depth(0)

        @pl.when(u == 5)
        def _():
            stats_plane(0)

    for m in (1, 2):
        own_block(m)
    stats_rows(1)
    finish(0)
    gather_start(0)
    stats_columns(1)
    gather_step(0, 1)
    stats_depth(1)
    gather_step(0, 2)
    gather_step(0, 3)
    stats_plane(1)
    gather_step(0, 4)
    finish(1)
    for m in (1, 2):
        gather_start(m)
    gather_step(0, 5)
    for m in (1, 2):
        gather_step(m, 1)
    gather_step(0, 6)
    for m in (1, 2):
        gather_step(m, 2)
    gather_step(0, 7)

    @pl.loop(3, 8)
    def _(s):
        for m in (1, 2):
            gather_step(m, s)

    @pl.loop(0, 8)
    def _(j):
        for m in range(3):

            @pl.when((near == 0) & (real(j, a) > 0))
            def _():
                for c in (0, 1):
                    raw_copy(m, real(j, a), c).wait_send()

            @pl.when((near >= 1) & (real(j, a) > near))
            def _():
                for c in (0, 1):
                    part_copy(m, a, near, real(j, a), c).wait_send()

            @pl.when(real(j, 1 - a) > far)
            def _():
                for c in (0, 1):
                    part_copy(m, 1 - a, far, real(j, 1 - a), c).wait_send()

            for d in (0, 1):
                held = (j <= k) if d == 0 else (j >= k)

                @pl.when(held & (k != 7 * (1 - d)))
                def _():
                    w_copy(m, d, j).wait_send()

    for b in (0, 1):
        for o in range(1, 4):
            y_copy(b, o).wait_send()
        for o in range(1, 8):
            p_copy(b, o).wait_send()

        @pl.loop(1, 16)
        def _(o):
            z_copy(b, o).wait_send()

        @pl.loop(1, 32)
        def _(o):
            f_copy(b, o).wait_send()


def results_kernel(*refs):
    copies = [pltpu.make_async_copy(refs[i], refs[15 + i], refs[30].at[i]) for i in range(9)]
    for copy in copies:
        copy.start()
    for m in range(3):
        refs[24 + m][...] = refs[9 + m][0, 0 : HEIGHTS[m]]
        refs[27 + m][...] = refs[12 + m][0, :]
    for copy in copies:
        copy.wait()


def body(*args):
    grads = [args[4 * m].reshape(N, HEIGHTS[m], WIDTHS[m]) for m in range(3)]
    masters = [args[4 * m + 1] for m in range(3)]
    rows = [args[4 * m + 2] for m in range(3)]
    columns = [args[4 * m + 3] for m in range(3)]
    shape = jax.ShapeDtypeStruct
    blocks = list(zip(HEIGHTS, WIDTHS))
    out_shape = (
        [shape(b, F32) for b in blocks]
        + [shape((N, *b), BF16) for b in blocks]
        + [shape((1, 128), F32)] * 3
        + [shape((1, w), F32) for w in WIDTHS]
        + [shape(b, F32) for b in blocks]
    )
    vmem = pl.BlockSpec(memory_space=pltpu.VMEM)
    dma = pltpu.SemaphoreType.DMA
    out = pl.pallas_call(
        kernel,
        out_shape=out_shape,
        in_specs=[pl.BlockSpec(memory_space=pltpu.HBM)] * 12,
        out_specs=[vmem] * 15,
        scratch_shapes=(
            [pltpu.VMEM((2, N, *b), F32) for b in blocks]
            + [pltpu.VMEM((2, N, *b), BF16) for b in blocks]
            + [pltpu.VMEM(b, F32) for b in blocks]
            + [pltpu.VMEM((h, 128), F32) for h in HEIGHTS]
            + [
                pltpu.VMEM((2, 8, 128), F32),
                pltpu.VMEM((2, 4, 8, 128), F32),
                pltpu.VMEM((2, 8, 8, 128), F32),
                pltpu.VMEM((2, 8, 8, 128), F32),
                pltpu.VMEM((2, 8, 128), F32),
                pltpu.VMEM((2, 16, 8, 128), F32),
                pltpu.VMEM((2, 8, 128), F32),
                pltpu.VMEM((2, 32, 8, 128), F32),
                pltpu.VMEM((2, 8, 8, 128), F32),
                dma((3, 2, 8, 2)),
                dma((3, 2, 8, 2)),
                dma((3, 2, 8)),
                dma((3, 8)),
                dma((2, 2, 4)),
                dma((2, 2, 8)),
                dma((2, 2, 16)),
                dma((2, 2, 32)),
            ]
            + [pltpu.VMEM((N, *b), BF16) for b in blocks]
            + [pltpu.VMEM(b, F32) for b in blocks]
            + [pltpu.VMEM((h,), F32) for h in HEIGHTS]
            + [pltpu.VMEM((w,), F32) for w in WIDTHS]
            + [dma((12,))]
        ),
        compiler_params=pltpu.CompilerParams(
            collective_id=0, has_side_effects=True, vmem_limit_bytes=28 * 1024 * 1024
        ),
    )(*[pltpu.with_memory_space_constraint(v, pltpu.HBM) for v in (*grads, *masters, *rows, *columns)])
    anywhere = pl.BlockSpec(memory_space=pl.ANY)
    final_shape = (
        [shape(b, F32) for b in blocks]
        + [shape((N, *b), BF16) for b in blocks]
        + [shape(b, F32) for b in blocks]
        + [shape((h,), F32) for h in HEIGHTS]
        + [shape((w,), F32) for w in WIDTHS]
    )
    big = list(out[0:6]) + list(out[12:15])
    final = pl.pallas_call(
        results_kernel,
        out_shape=final_shape,
        in_specs=[vmem] * 15,
        out_specs=[anywhere] * 9 + [vmem] * 6,
        scratch_shapes=[dma((9,))],
        compiler_params=pltpu.CompilerParams(vmem_limit_bytes=8 * 1024 * 1024),
    )(*big, *out[6:12])
    result = []
    for m in range(3):
        result += [final[m], final[3 + m].reshape(N * HEIGHTS[m], WIDTHS[m]), final[9 + m], final[12 + m], final[6 + m]]
    return tuple(result)


def solution(mesh):
    finer = Mesh(mesh.devices.reshape(mesh.shape["dp"], 2, 4, 2, mesh.shape["col"]), ("dp", *ROW, "col"))
    one = (P("dp", ROW, "col"), P(ROW_DP, "col"), P(ROW_DP), P("col"))
    back = (P(ROW_DP, "col"), P(ROW, "col"), P(ROW_DP), P("col"), P(ROW_DP, "col"))
    return jax.shard_map(body, mesh=finer, in_specs=one * 3, out_specs=back * 3, check_vma=False)
```

```python
import jax
import jax.numpy as jnp
from jax import lax
from jax.experimental import pallas as pl
from jax.experimental.pallas import tpu as pltpu
from jax.sharding import Mesh
from jax.sharding import PartitionSpec as P

MESH = pl.DeviceIdType.MESH
F32 = jnp.float32
BF16 = jnp.bfloat16

ROW = ("zhi", "x", "core")
ROW_DP = ("zhi", "x", "core", "dp")

tiny_square = 1e-30
decay_rate = 0.9
learn_rate = 0.01

N = 8
HEIGHTS = (32, 40, 32)
WIDTHS = (1280, 1024, 1024)
FULL_ROWS = (4096, 5120, 4096)
FULL_COLS = (5120, 4096, 4096)
BATCHES = ((0,), (1, 2))
LAYOUT = (((0, 0, 0, 8), (1, 0, 8, 10)), ((0, 1, 0, 8), (1, 2, 0, 8)))


def remote(src, dst, send_sem, recv_sem, device):
    return pltpu.make_async_remote_copy(
        src_ref=src, dst_ref=dst, send_sem=send_sem, recv_sem=recv_sem, device_id=device, device_id_type=MESH
    )


def to_column(row, height):
    sub = lax.broadcasted_iota(jnp.int32, (height, 128), 0)
    lane = lax.broadcasted_iota(jnp.int32, (height, 128), 1)
    return jnp.sum(jnp.where(sub == lane, jnp.broadcast_to(row, (height, 128)), 0.0), axis=1, keepdims=True)


def to_row(column, height):
    sub = lax.broadcasted_iota(jnp.int32, (height, 128), 0)
    lane = lax.broadcasted_iota(jnp.int32, (height, 128), 1)
    return jnp.sum(jnp.where(sub == lane, jnp.broadcast_to(column, (height, 128)), 0.0), axis=0, keepdims=True)


def as_row(ref, height):
    return jnp.pad(ref[...].reshape(1, height), ((0, 0), (0, 128 - height)))


def kernel(*refs):
    given = refs[0:12]
    updated, weights, rows_next, columns_next, steps = refs[12:15], refs[15:18], refs[18:21], refs[21:24], refs[24:27]
    (
        part0, part1, part2, raw0, raw1, raw2, acc0, acc1, acc2,
        rfac0, rfac1, rfac2,
        ysend, yrecv, piece, pieces_in, zsend, zrecv, total, fin, ratios, colstat,
        rs_send, rs_recv, ag_send, ag_recv, y_sems, p_sems, z_sems, f_sems,
        *held, load_sems,
    ) = refs[27:]
    grads, masters, rows, columns = held[0:3], held[3:6], held[6:9], held[9:12]
    loads = [pltpu.make_async_copy(given[i], held[i], load_sems.at[i]) for i in range(12)]
    parts, raws, accs, rfacs = (part0, part1, part2), (raw0, raw1, raw2), (acc0, acc1, acc2), (rfac0, rfac1, rfac2)

    k = lax.axis_index("dp")
    zhi, x, core, y = lax.axis_index("zhi"), lax.axis_index("x"), lax.axis_index("core"), lax.axis_index("col")
    p = x * 2 + core
    q = zhi * 8 + k
    n = y * 8 + p

    def z_peer(o):
        t = lax.rem(q + o, 16)
        return {"zhi": t // 8, "dp": lax.rem(t, 8)}

    def p_peer(t):
        return {"x": t // 2, "core": lax.rem(t, 2)}

    def plane_peer(o):
        t = lax.rem(n + o, 32)
        s = lax.rem(t, 8)
        return {"x": s // 2, "core": lax.rem(s, 2), "col": t // 8}

    barrier = pltpu.get_barrier_semaphore()

    def far_first(i):
        return jnp.where(lax.rem(i, 2) == 1, 8 - (i + 1) // 2, 8 + i // 2)

    @pl.loop(0, 15)
    def _(i):
        pl.semaphore_signal(barrier, inc=1, device_id=z_peer(far_first(i)), device_id_type=MESH)

    @pl.loop(1, 32)
    def _(o):
        pl.semaphore_signal(barrier, inc=1, device_id=plane_peer(o), device_id_type=MESH)

    for load in loads:
        load.start()
    for load in loads:
        load.wait()
    pl.semaphore_wait(barrier, 46)

    a = k // 4
    near = jnp.where(a == 0, k, 7 - k)
    far = 7 - near

    def real(jd, d):
        return jd + d * (7 - 2 * jd)

    def half(m, c):
        return pl.ds(c * (WIDTHS[m] // 2), WIDTHS[m] // 2)

    def raw_copy(m, jd, c):
        j = real(jd, a)
        return remote(
            grads[m].at[j, :, half(m, c)], raws[m].at[a, j, :, half(m, c)], rs_send.at[m, a, j, c],
            rs_recv.at[m, a, j, c], {"dp": real(1, a)},
        )

    def part_copy(m, d, here, jd, c):
        j = real(jd, d)
        block = parts[m].at[d, j, :, half(m, c)]
        return remote(
            block, block, rs_send.at[m, d, j, c], rs_recv.at[m, d, j, c], {"dp": real(jnp.minimum(here + 1, 7), d)}
        )

    def send_raw(m):
        @pl.when(near == 0)
        def _():
            @pl.loop(0, 7)
            def _(s):
                for c in (0, 1):
                    raw_copy(m, 7 - s, c).start()

    def forward_first(m, jd, c):
        j = real(jd, a)
        cut = half(m, c)

        @pl.when((near == 1) & (jd > near))
        def _():
            raw_copy(m, jd, c).wait_recv()
            parts[m][a, j, :, cut] = raws[m][a, j, :, cut].astype(F32) + grads[m][j, :, cut].astype(F32)
            part_copy(m, a, near, jd, c).start()

        @pl.when((near >= 2) & (jd > near))
        def _():
            forward_part(m, a, near, jd, c)

    def forward_part(m, d, here, jd, c):
        j = real(jd, d)
        cut = half(m, c)
        part_copy(m, d, here, jd, c).wait_recv()
        parts[m][d, j, :, cut] = parts[m][d, j, :, cut] + grads[m][j, :, cut].astype(F32)
        part_copy(m, d, here, jd, c).start()

    def forward_second(m, r, c):
        @pl.when((r >= 0) & (7 - r > far))
        def _():
            forward_part(m, 1 - a, far, 7 - r, c)

    def forward(ms, u, behind):
        for m in ms:
            for c in (0, 1):
                forward_first(m, 7 - u, c)
                forward_second(m, u - behind, c)

    def own_block(m):
        b = 1 - a
        for c in (0, 1):
            part_copy(m, b, far, far, c).wait_recv()
        accs[m][...] = parts[m][b, k] + grads[m][k].astype(F32)

        @pl.when(near == 1)
        def _():
            for c in (0, 1):
                raw_copy(m, near, c).wait_recv()
            accs[m][...] = accs[m][...] + raws[m][a, k].astype(F32)

        @pl.when(near >= 2)
        def _():
            for c in (0, 1):
                part_copy(m, a, near, near, c).wait_recv()
            accs[m][...] = accs[m][...] + parts[m][a, k]

        accs[m][...] = accs[m][...] * 0.125

    def y_copy(b, o):
        t = lax.rem(y + o, 4)
        return remote(ysend.at[b], yrecv.at[b, o], y_sems.at[0, b, o], y_sems.at[1, b, o], {"col": t})

    def stats_rows(b):
        for at_row, m in enumerate(BATCHES[b]):
            square = accs[m][...] * accs[m][...] + tiny_square
            total_row = jnp.sum(square, axis=1, keepdims=True)
            ysend[b, at_row : at_row + 1] = to_row(total_row, HEIGHTS[m])
        for o in range(1, 4):
            y_copy(b, o).start()

    def p_copy(b, o):
        t = lax.rem(p + o, 8)
        return remote(piece.at[b, t], pieces_in.at[b, o], p_sems.at[0, b, o], p_sems.at[1, b, o], p_peer(t))

    def stats_columns(b):
        for o in range(1, 4):
            y_copy(b, o).wait_recv()
        piece[b] = jnp.zeros((8, 8, 128), F32)
        for m in BATCHES[b]:
            height = HEIGHTS[m]
            at = slice(BATCHES[b].index(m), BATCHES[b].index(m) + 1)
            across = (ysend[b, at] + yrecv[b, 1, at]) + (yrecv[b, 2, at] + yrecv[b, 3, at])
            new = decay_rate * as_row(rows[m], height) + (1.0 - decay_rate) * (across / FULL_COLS[m])
            rows_next[m][...] = new
            new_column = to_column(new, height)
            rfacs[m][...] = jnp.broadcast_to(new_column, (height, 128))
            row_sum = jnp.broadcast_to(jnp.sum(new_column, axis=0, keepdims=True), (1, 128))
            g = accs[m][...]
            square = g * g
            plain = jnp.sum(square + tiny_square, axis=0, keepdims=True)
            weighted = jnp.sum(square * (1.0 / new_column), axis=0, keepdims=True)
            for slot, owner, lo, hi in LAYOUT[b]:
                if owner != m:
                    continue
                for group in range(lo, hi):
                    cut = slice(128 * group, 128 * group + 128)
                    piece[b, group - lo, 2 * slot : 2 * slot + 1] = plain[:, cut]
                    piece[b, group - lo, 2 * slot + 1 : 2 * slot + 2] = weighted[:, cut]
            at_row = 7 - BATCHES[b].index(m)
            for which in range(8):
                piece[b, which, at_row : at_row + 1] = row_sum
        for o in range(1, 8):
            p_copy(b, o).start()

    def z_copy(b, o):
        return remote(zsend.at[b], zrecv.at[b, o], z_sems.at[0, b, o], z_sems.at[1, b, o], z_peer(o))

    def stats_depth(b):
        tile = piece[b, p]
        for o in range(1, 8):
            p_copy(b, o).wait_recv()
            tile = tile + pieces_in[b, o]
        zsend[b] = tile

        @pl.loop(0, 15)
        def _(i):
            z_copy(b, far_first(i)).start()

        colstat[b] = jnp.ones((8, 8, 128), F32)
        for slot, m, lo, hi in LAYOUT[b]:
            for group in range(lo, hi):
                cut = slice(128 * group, 128 * group + 128)
                colstat[b, group - lo, 2 * slot : 2 * slot + 1] = columns[m][cut].reshape(1, 128)

    def f_copy(b, o):
        t = lax.rem(p + o, 8)
        return remote(fin.at[b, p], fin.at[b, p], f_sems.at[0, b, o], f_sems.at[1, b, o], p_peer(t))

    def g_copy(b, i):
        t = lax.rem(p + lax.rem(i, 8), 8)
        peer = {"x": t // 2, "core": lax.rem(t, 2), "col": lax.rem(y + i // 8, 4)}
        return remote(ratios.at[b, 0], ratios.at[b, i], f_sems.at[0, b, i], f_sems.at[1, b, i], peer)

    def next_column(old, total_square, m):
        return decay_rate * old + (1.0 - decay_rate) * (total_square / FULL_ROWS[m])

    def stats_plane(b):
        @pl.loop(1, 16)
        def _(o):
            z_copy(b, o).wait_recv()

        tile = zsend[b]
        for o in range(1, 16):
            tile = tile + zrecv[b, o]
        total[b] = tile
        fin[b, p] = tile
        lane = lax.broadcasted_iota(jnp.int32, (1, 128), 1)
        marks = jnp.zeros((1, 128), F32)
        for slot, m, lo, hi in LAYOUT[b]:
            plain = total[b, 2 * slot : 2 * slot + 1]
            weighted = total[b, 2 * slot + 1 : 2 * slot + 2]
            new = next_column(colstat[b, p, 2 * slot : 2 * slot + 1], plain, m)
            ratio = jnp.sum(weighted / new, axis=1, keepdims=True)
            marks = marks + jnp.where(lane == slot, jnp.broadcast_to(ratio, (1, 128)), 0.0)
        ratios[b, 0] = marks
        fin[b, p, 5:6] = marks

        @pl.loop(0, 8)
        def _(o):
            g_copy(b, 16 + o).start()

        @pl.loop(0, 8)
        def _(o):
            g_copy(b, 8 + o).start()
            g_copy(b, 24 + o).start()

        @pl.loop(1, 8)
        def _(o):
            f_copy(b, o).start()

    def finish(b):
        @pl.loop(1, 8)
        def _(o):
            f_copy(b, o).wait_recv()

        @pl.loop(8, 32)
        def _(i):
            g_copy(b, i).wait_recv()

        everyone = fin[b, 0, 5:6]
        for which in range(1, 8):
            everyone = everyone + fin[b, which, 5:6]
        for which in range(8, 32):
            everyone = everyone + ratios[b, which]
        lane = lax.broadcasted_iota(jnp.int32, (1, 128), 1)
        for m in BATCHES[b]:
            for slot, owner, lo, hi in LAYOUT[b]:
                if owner != m:
                    continue
                for group in range(lo, hi):
                    cut = slice(128 * group, 128 * group + 128)
                    plain = fin[b, group - lo, 2 * slot : 2 * slot + 1]
                    columns_next[m][:, cut] = next_column(columns[m][cut].reshape(1, 128), plain, m)
            at_row = 7 - BATCHES[b].index(m)
            row_mean = total[b, at_row : at_row + 1] / FULL_ROWS[m]
            mine = [slot for slot, owner, _, _ in LAYOUT[b] if owner == m]
            chosen = lane == mine[0]
            for slot in mine[1:]:
                chosen = chosen | (lane == slot)
            ratio = jnp.sum(jnp.where(chosen, everyone, 0.0), axis=1, keepdims=True)
            mean_square = row_mean * ratio / (FULL_ROWS[m] * FULL_COLS[m])
            clip = jnp.maximum(1.0, jnp.sqrt(mean_square))
            row_scale = (jnp.sqrt(row_mean) / clip) / jnp.sqrt(rfacs[m][...])
            column_scale = 1.0 / jnp.sqrt(columns_next[m][...])
            step = accs[m][...] * row_scale[:, 0:1] * column_scale
            steps[m][...] = step
            new = masters[m][...] - learn_rate * step
            updated[m][...] = new
            weights[m][k] = new.astype(BF16)

    def w_copy(m, d, i):
        to = jnp.clip(k + 1 - 2 * d, 0, 7)
        return remote(weights[m].at[i], weights[m].at[i], ag_send.at[m, d, i], ag_recv.at[m, i], {"dp": to})

    def gather_start(m):
        for d in (0, 1):

            @pl.when(k != 7 * (1 - d))
            def _():
                w_copy(m, d, k).start()

    def gather_step(m, s):
        for d in (0, 1):
            i = k - s if d == 0 else k + s

            @pl.when((i >= 0) & (i <= 7))
            def _():
                w_copy(m, d, i).wait_recv()

                @pl.when(k != 7 * (1 - d))
                def _():
                    w_copy(m, d, i).start()

    for m in range(3):
        send_raw(m)

    lag = jnp.where(near == 1, 6, jnp.where(near == 2, 4, 2))
    lag_pair = jnp.where(near == 1, 6, jnp.where(near == 2, 2, 1))

    @pl.loop(0, 8)
    def _(u):
        forward((0,), u, lag)

    @pl.loop(0, 8)
    def _(u):
        @pl.when(u == 3 - near)
        def _():
            own_block(0)
            stats_rows(0)

        @pl.when(u == 4 - near)
        def _():
            stats_columns(0)

        @pl.when(u == 5 - near)
        def _():
            stats_depth(0)

        forward((1, 2), u, lag_pair)

    stats_plane(0)
    for m in (1, 2):
        own_block(m)
    stats_rows(1)
    finish(0)
    gather_start(0)
    stats_columns(1)
    gather_step(0, 1)
    stats_depth(1)
    gather_step(0, 2)
    gather_step(0, 3)
    stats_plane(1)
    gather_step(0, 4)
    gather_step(0, 5)
    finish(1)
    for m in (1, 2):
        gather_start(m)
    gather_step(0, 6)
    for m in (1, 2):
        gather_step(m, 1)
    gather_step(0, 7)
    for m in (1, 2):
        gather_step(m, 2)

    @pl.loop(3, 8)
    def _(s):
        for m in (1, 2):
            gather_step(m, s)

    @pl.loop(0, 8)
    def _(j):
        for m in range(3):

            @pl.when((near == 0) & (real(j, a) > 0))
            def _():
                for c in (0, 1):
                    raw_copy(m, real(j, a), c).wait_send()

            @pl.when((near >= 1) & (real(j, a) > near))
            def _():
                for c in (0, 1):
                    part_copy(m, a, near, real(j, a), c).wait_send()

            @pl.when(real(j, 1 - a) > far)
            def _():
                for c in (0, 1):
                    part_copy(m, 1 - a, far, real(j, 1 - a), c).wait_send()

            for d in (0, 1):
                held = (j <= k) if d == 0 else (j >= k)

                @pl.when(held & (k != 7 * (1 - d)))
                def _():
                    w_copy(m, d, j).wait_send()

    for b in (0, 1):
        for o in range(1, 4):
            y_copy(b, o).wait_send()
        for o in range(1, 8):
            p_copy(b, o).wait_send()

        @pl.loop(1, 16)
        def _(o):
            z_copy(b, o).wait_send()

        @pl.loop(1, 8)
        def _(o):
            f_copy(b, o).wait_send()

        @pl.loop(8, 32)
        def _(i):
            g_copy(b, i).wait_send()


def results_kernel(*refs):
    copies = [pltpu.make_async_copy(refs[i], refs[15 + i], refs[30].at[i]) for i in range(9)]
    for copy in copies:
        copy.start()
    for m in range(3):
        refs[24 + m][...] = refs[9 + m][0, 0 : HEIGHTS[m]]
        refs[27 + m][...] = refs[12 + m][0, :]
    for copy in copies:
        copy.wait()


def body(*args):
    grads = [args[4 * m].reshape(N, HEIGHTS[m], WIDTHS[m]) for m in range(3)]
    masters = [args[4 * m + 1] for m in range(3)]
    rows = [args[4 * m + 2] for m in range(3)]
    columns = [args[4 * m + 3] for m in range(3)]
    shape = jax.ShapeDtypeStruct
    blocks = list(zip(HEIGHTS, WIDTHS))
    out_shape = (
        [shape(b, F32) for b in blocks]
        + [shape((N, *b), BF16) for b in blocks]
        + [shape((1, 128), F32)] * 3
        + [shape((1, w), F32) for w in WIDTHS]
        + [shape(b, F32) for b in blocks]
    )
    vmem = pl.BlockSpec(memory_space=pltpu.VMEM)
    dma = pltpu.SemaphoreType.DMA
    out = pl.pallas_call(
        kernel,
        out_shape=out_shape,
        in_specs=[pl.BlockSpec(memory_space=pltpu.HBM)] * 12,
        out_specs=[vmem] * 15,
        scratch_shapes=(
            [pltpu.VMEM((2, N, *b), F32) for b in blocks]
            + [pltpu.VMEM((2, N, *b), BF16) for b in blocks]
            + [pltpu.VMEM(b, F32) for b in blocks]
            + [pltpu.VMEM((h, 128), F32) for h in HEIGHTS]
            + [
                pltpu.VMEM((2, 8, 128), F32),
                pltpu.VMEM((2, 4, 8, 128), F32),
                pltpu.VMEM((2, 8, 8, 128), F32),
                pltpu.VMEM((2, 8, 8, 128), F32),
                pltpu.VMEM((2, 8, 128), F32),
                pltpu.VMEM((2, 16, 8, 128), F32),
                pltpu.VMEM((2, 8, 128), F32),
                pltpu.VMEM((2, 8, 8, 128), F32),
                pltpu.VMEM((2, 32, 1, 128), F32),
                pltpu.VMEM((2, 8, 8, 128), F32),
                dma((3, 2, 8, 2)),
                dma((3, 2, 8, 2)),
                dma((3, 2, 8)),
                dma((3, 8)),
                dma((2, 2, 4)),
                dma((2, 2, 8)),
                dma((2, 2, 16)),
                dma((2, 2, 32)),
            ]
            + [pltpu.VMEM((N, *b), BF16) for b in blocks]
            + [pltpu.VMEM(b, F32) for b in blocks]
            + [pltpu.VMEM((h,), F32) for h in HEIGHTS]
            + [pltpu.VMEM((w,), F32) for w in WIDTHS]
            + [dma((12,))]
        ),
        compiler_params=pltpu.CompilerParams(
            collective_id=0, has_side_effects=True, vmem_limit_bytes=28 * 1024 * 1024
        ),
    )(*[pltpu.with_memory_space_constraint(v, pltpu.HBM) for v in (*grads, *masters, *rows, *columns)])
    anywhere = pl.BlockSpec(memory_space=pl.ANY)
    final_shape = (
        [shape(b, F32) for b in blocks]
        + [shape((N, *b), BF16) for b in blocks]
        + [shape(b, F32) for b in blocks]
        + [shape((h,), F32) for h in HEIGHTS]
        + [shape((w,), F32) for w in WIDTHS]
    )
    big = list(out[0:6]) + list(out[12:15])
    final = pl.pallas_call(
        results_kernel,
        out_shape=final_shape,
        in_specs=[vmem] * 15,
        out_specs=[anywhere] * 9 + [vmem] * 6,
        scratch_shapes=[dma((9,))],
        compiler_params=pltpu.CompilerParams(vmem_limit_bytes=8 * 1024 * 1024),
    )(*big, *out[6:12])
    result = []
    for m in range(3):
        result += [final[m], final[3 + m].reshape(N * HEIGHTS[m], WIDTHS[m]), final[9 + m], final[12 + m], final[6 + m]]
    return tuple(result)


def solution(mesh):
    finer = Mesh(mesh.devices.reshape(mesh.shape["dp"], 2, 4, 2, mesh.shape["col"]), ("dp", *ROW, "col"))
    one = (P("dp", ROW, "col"), P(ROW_DP, "col"), P(ROW_DP), P("col"))
    back = (P(ROW_DP, "col"), P(ROW, "col"), P(ROW_DP), P("col"), P(ROW_DP, "col"))
    return jax.shard_map(body, mesh=finer, in_specs=one * 3, out_specs=back * 3, check_vma=False)
```

```python
import jax
import jax.numpy as jnp
from jax import lax
from jax.experimental import pallas as pl
from jax.experimental.pallas import tpu as pltpu
from jax.sharding import Mesh
from jax.sharding import PartitionSpec as P

MESH = pl.DeviceIdType.MESH
F32 = jnp.float32
BF16 = jnp.bfloat16

ROW = ("zhi", "x", "core")
ROW_DP = ("zhi", "x", "core", "dp")

tiny_square = 1e-30
decay_rate = 0.9
learn_rate = 0.01

N = 8
HEIGHTS = (32, 40, 32)
WIDTHS = (1280, 1024, 1024)
FULL_ROWS = (4096, 5120, 4096)
FULL_COLS = (5120, 4096, 4096)
BATCHES = ((0,), (1, 2))
LAYOUT = (((0, 0, 0, 8), (1, 0, 8, 10)), ((0, 1, 0, 8), (1, 2, 0, 8)))


def remote(src, dst, send_sem, recv_sem, device):
    return pltpu.make_async_remote_copy(
        src_ref=src, dst_ref=dst, send_sem=send_sem, recv_sem=recv_sem, device_id=device, device_id_type=MESH
    )


def to_column(row, height):
    sub = lax.broadcasted_iota(jnp.int32, (height, 128), 0)
    lane = lax.broadcasted_iota(jnp.int32, (height, 128), 1)
    return jnp.sum(jnp.where(sub == lane, jnp.broadcast_to(row, (height, 128)), 0.0), axis=1, keepdims=True)


def to_row(column, height):
    sub = lax.broadcasted_iota(jnp.int32, (height, 128), 0)
    lane = lax.broadcasted_iota(jnp.int32, (height, 128), 1)
    return jnp.sum(jnp.where(sub == lane, jnp.broadcast_to(column, (height, 128)), 0.0), axis=0, keepdims=True)


def as_row(ref, height):
    return jnp.pad(ref[...].reshape(1, height), ((0, 0), (0, 128 - height)))


def kernel(*refs):
    given = refs[0:12]
    updated, weights, rows_next, columns_next, steps = refs[12:15], refs[15:18], refs[18:21], refs[21:24], refs[24:27]
    (
        part0, part1, part2, raw0, raw1, raw2, acc0, acc1, acc2,
        rfac0, rfac1, rfac2,
        ysend, yrecv, piece, pieces_in, zsend, zrecv, total, fin, ratios, colstat,
        rs_send, rs_recv, ag_send, ag_recv, y_sems, p_sems, z_sems, f_sems,
        *held, load_sems,
    ) = refs[27:]
    grads, masters, rows, columns = held[0:3], held[3:6], held[6:9], held[9:12]
    loads = [pltpu.make_async_copy(given[i], held[i], load_sems.at[i]) for i in range(12)]
    parts, raws, accs, rfacs = (part0, part1, part2), (raw0, raw1, raw2), (acc0, acc1, acc2), (rfac0, rfac1, rfac2)

    k = lax.axis_index("dp")
    zhi, x, core, y = lax.axis_index("zhi"), lax.axis_index("x"), lax.axis_index("core"), lax.axis_index("col")
    p = x * 2 + core
    q = zhi * 8 + k
    n = y * 8 + p

    def z_peer(o):
        t = lax.rem(q + o, 16)
        return {"zhi": t // 8, "dp": lax.rem(t, 8)}

    def p_peer(t):
        return {"x": t // 2, "core": lax.rem(t, 2)}

    def plane_peer(o):
        t = lax.rem(n + o, 32)
        s = lax.rem(t, 8)
        return {"x": s // 2, "core": lax.rem(s, 2), "col": t // 8}

    barrier = pltpu.get_barrier_semaphore()

    def far_first(i):
        return jnp.where(lax.rem(i, 2) == 1, 8 - (i + 1) // 2, 8 + i // 2)

    @pl.loop(0, 15)
    def _(i):
        pl.semaphore_signal(barrier, inc=1, device_id=z_peer(far_first(i)), device_id_type=MESH)

    @pl.loop(1, 32)
    def _(o):
        pl.semaphore_signal(barrier, inc=1, device_id=plane_peer(o), device_id_type=MESH)

    for load in loads:
        load.start()
    for load in loads:
        load.wait()
    pl.semaphore_wait(barrier, 46)

    a = k // 4
    near = jnp.where(a == 0, k, 7 - k)
    far = 7 - near

    def real(jd, d):
        return jd + d * (7 - 2 * jd)

    def half(m, c):
        return pl.ds(c * (WIDTHS[m] // 2), WIDTHS[m] // 2)

    def raw_copy(m, jd, c):
        j = real(jd, a)
        return remote(
            grads[m].at[j, :, half(m, c)], raws[m].at[a, j, :, half(m, c)], rs_send.at[m, a, j, c],
            rs_recv.at[m, a, j, c], {"dp": real(1, a)},
        )

    def part_copy(m, d, here, jd, c):
        j = real(jd, d)
        block = parts[m].at[d, j, :, half(m, c)]
        return remote(
            block, block, rs_send.at[m, d, j, c], rs_recv.at[m, d, j, c], {"dp": real(jnp.minimum(here + 1, 7), d)}
        )

    def send_raw(m):
        @pl.when(near == 0)
        def _():
            @pl.loop(0, 7)
            def _(s):
                for c in (0, 1):
                    raw_copy(m, 7 - s, c).start()

    def forward_first(m, jd, c):
        j = real(jd, a)
        cut = half(m, c)

        @pl.when((near == 1) & (jd > near))
        def _():
            raw_copy(m, jd, c).wait_recv()
            parts[m][a, j, :, cut] = raws[m][a, j, :, cut].astype(F32) + grads[m][j, :, cut].astype(F32)
            part_copy(m, a, near, jd, c).start()

        @pl.when((near >= 2) & (jd > near))
        def _():
            forward_part(m, a, near, jd, c)

    def forward_part(m, d, here, jd, c):
        j = real(jd, d)
        cut = half(m, c)
        part_copy(m, d, here, jd, c).wait_recv()
        parts[m][d, j, :, cut] = parts[m][d, j, :, cut] + grads[m][j, :, cut].astype(F32)
        part_copy(m, d, here, jd, c).start()

    def forward_second(m, r, c):
        @pl.when((r >= 0) & (7 - r > far))
        def _():
            forward_part(m, 1 - a, far, 7 - r, c)

    def forward(ms, u, behind):
        for m in ms:
            for c in (0, 1):
                forward_first(m, 7 - u, c)
                forward_second(m, u - behind, c)

    def own_block(m):
        b = 1 - a
        for c in (0, 1):
            part_copy(m, b, far, far, c).wait_recv()
        accs[m][...] = parts[m][b, k] + grads[m][k].astype(F32)

        @pl.when(near == 1)
        def _():
            for c in (0, 1):
                raw_copy(m, near, c).wait_recv()
            accs[m][...] = accs[m][...] + raws[m][a, k].astype(F32)

        @pl.when(near >= 2)
        def _():
            for c in (0, 1):
                part_copy(m, a, near, near, c).wait_recv()
            accs[m][...] = accs[m][...] + parts[m][a, k]

        accs[m][...] = accs[m][...] * 0.125

    def y_copy(b, o):
        t = lax.rem(y + o, 4)
        return remote(ysend.at[b], yrecv.at[b, o], y_sems.at[0, b, o], y_sems.at[1, b, o], {"col": t})

    def stats_rows(b):
        for at_row, m in enumerate(BATCHES[b]):
            square = accs[m][...] * accs[m][...] + tiny_square
            total_row = jnp.sum(square, axis=1, keepdims=True)
            ysend[b, at_row : at_row + 1] = to_row(total_row, HEIGHTS[m])
        for o in range(1, 4):
            y_copy(b, o).start()

    def p_copy(b, o):
        t = lax.rem(p + o, 8)
        return remote(piece.at[b, t], pieces_in.at[b, o], p_sems.at[0, b, o], p_sems.at[1, b, o], p_peer(t))

    def stats_columns(b):
        for o in range(1, 4):
            y_copy(b, o).wait_recv()
        piece[b] = jnp.zeros((8, 8, 128), F32)
        for m in BATCHES[b]:
            height = HEIGHTS[m]
            at = slice(BATCHES[b].index(m), BATCHES[b].index(m) + 1)
            across = (ysend[b, at] + yrecv[b, 1, at]) + (yrecv[b, 2, at] + yrecv[b, 3, at])
            new = decay_rate * as_row(rows[m], height) + (1.0 - decay_rate) * (across / FULL_COLS[m])
            rows_next[m][...] = new
            new_column = to_column(new, height)
            rfacs[m][...] = jnp.broadcast_to(new_column, (height, 128))
            row_sum = jnp.broadcast_to(jnp.sum(new_column, axis=0, keepdims=True), (1, 128))
            g = accs[m][...]
            square = g * g
            plain = jnp.sum(square + tiny_square, axis=0, keepdims=True)
            weighted = jnp.sum(square * (1.0 / new_column), axis=0, keepdims=True)
            for slot, owner, lo, hi in LAYOUT[b]:
                if owner != m:
                    continue
                for group in range(lo, hi):
                    cut = slice(128 * group, 128 * group + 128)
                    piece[b, group - lo, 2 * slot : 2 * slot + 1] = plain[:, cut]
                    piece[b, group - lo, 2 * slot + 1 : 2 * slot + 2] = weighted[:, cut]
            at_row = 7 - BATCHES[b].index(m)
            for which in range(8):
                piece[b, which, at_row : at_row + 1] = row_sum
        for o in range(1, 8):
            p_copy(b, o).start()

    def z_copy(b, o):
        return remote(zsend.at[b], zrecv.at[b, o], z_sems.at[0, b, o], z_sems.at[1, b, o], z_peer(o))

    def stats_depth(b):
        tile = piece[b, p]
        for o in range(1, 8):
            p_copy(b, o).wait_recv()
            tile = tile + pieces_in[b, o]
        zsend[b] = tile

        @pl.loop(0, 15)
        def _(i):
            z_copy(b, far_first(i)).start()

        colstat[b] = jnp.ones((8, 8, 128), F32)
        for slot, m, lo, hi in LAYOUT[b]:
            for group in range(lo, hi):
                cut = slice(128 * group, 128 * group + 128)
                colstat[b, group - lo, 2 * slot : 2 * slot + 1] = columns[m][cut].reshape(1, 128)

    def f_copy(b, o):
        t = lax.rem(p + o, 8)
        return remote(fin.at[b, p], fin.at[b, p], f_sems.at[0, b, o], f_sems.at[1, b, o], p_peer(t))

    def g_copy(b, i):
        t = lax.rem(p + lax.rem(i, 8), 8)
        peer = {"x": t // 2, "core": lax.rem(t, 2), "col": lax.rem(y + i // 8, 4)}
        return remote(ratios.at[b, 0], ratios.at[b, i], f_sems.at[0, b, i], f_sems.at[1, b, i], peer)

    def next_column(old, total_square, m):
        return decay_rate * old + (1.0 - decay_rate) * (total_square / FULL_ROWS[m])

    def stats_plane(b):
        @pl.loop(1, 16)
        def _(o):
            z_copy(b, o).wait_recv()

        tile = zsend[b]
        for o in range(1, 16):
            tile = tile + zrecv[b, o]
        total[b] = tile
        fin[b, p] = tile
        lane = lax.broadcasted_iota(jnp.int32, (1, 128), 1)
        marks = jnp.zeros((1, 128), F32)
        for slot, m, lo, hi in LAYOUT[b]:
            plain = total[b, 2 * slot : 2 * slot + 1]
            weighted = total[b, 2 * slot + 1 : 2 * slot + 2]
            new = next_column(colstat[b, p, 2 * slot : 2 * slot + 1], plain, m)
            ratio = jnp.sum(weighted / new, axis=1, keepdims=True)
            marks = marks + jnp.where(lane == slot, jnp.broadcast_to(ratio, (1, 128)), 0.0)
        ratios[b, 0] = marks
        fin[b, p, 5:6] = marks

        @pl.loop(0, 8)
        def _(o):
            g_copy(b, 16 + o).start()

        @pl.loop(0, 8)
        def _(o):
            g_copy(b, 8 + o).start()
            g_copy(b, 24 + o).start()

        @pl.loop(1, 8)
        def _(o):
            f_copy(b, o).start()

    def finish(b):
        @pl.loop(1, 8)
        def _(o):
            f_copy(b, o).wait_recv()

        @pl.loop(8, 32)
        def _(i):
            g_copy(b, i).wait_recv()

        everyone = fin[b, 0, 5:6]
        for which in range(1, 8):
            everyone = everyone + fin[b, which, 5:6]
        for which in range(8, 32):
            everyone = everyone + ratios[b, which]
        lane = lax.broadcasted_iota(jnp.int32, (1, 128), 1)
        for m in BATCHES[b]:
            for slot, owner, lo, hi in LAYOUT[b]:
                if owner != m:
                    continue
                for group in range(lo, hi):
                    cut = slice(128 * group, 128 * group + 128)
                    plain = fin[b, group - lo, 2 * slot : 2 * slot + 1]
                    columns_next[m][:, cut] = next_column(columns[m][cut].reshape(1, 128), plain, m)
            at_row = 7 - BATCHES[b].index(m)
            row_mean = total[b, at_row : at_row + 1] / FULL_ROWS[m]
            mine = [slot for slot, owner, _, _ in LAYOUT[b] if owner == m]
            chosen = lane == mine[0]
            for slot in mine[1:]:
                chosen = chosen | (lane == slot)
            ratio = jnp.sum(jnp.where(chosen, everyone, 0.0), axis=1, keepdims=True)
            mean_square = row_mean * ratio / (FULL_ROWS[m] * FULL_COLS[m])
            clip = jnp.maximum(1.0, jnp.sqrt(mean_square))
            row_scale = (jnp.sqrt(row_mean) / clip) / jnp.sqrt(rfacs[m][...])
            column_scale = 1.0 / jnp.sqrt(columns_next[m][...])
            step = accs[m][...] * row_scale[:, 0:1] * column_scale
            steps[m][...] = step
            new = masters[m][...] - learn_rate * step
            updated[m][...] = new
            weights[m][k] = new.astype(BF16)

    def w_copy(m, d, i):
        to = jnp.clip(k + 1 - 2 * d, 0, 7)
        return remote(weights[m].at[i], weights[m].at[i], ag_send.at[m, d, i], ag_recv.at[m, i], {"dp": to})

    def gather_start(m):
        for d in (0, 1):

            @pl.when(k != 7 * (1 - d))
            def _():
                w_copy(m, d, k).start()

    def gather_step(m, s):
        for d in (0, 1):
            i = k - s if d == 0 else k + s

            @pl.when((i >= 0) & (i <= 7))
            def _():
                w_copy(m, d, i).wait_recv()

                @pl.when(k != 7 * (1 - d))
                def _():
                    w_copy(m, d, i).start()

    for m in range(3):
        send_raw(m)

    lag = jnp.where(near == 1, 6, jnp.where(near == 2, 4, 2))
    lag_pair = jnp.where(near == 1, 6, jnp.where(near == 2, 2, 1))

    @pl.loop(0, 8)
    def _(u):
        forward((0,), u, lag)

    @pl.loop(0, 8)
    def _(u):
        @pl.when(u == 3 - near)
        def _():
            own_block(0)
            stats_rows(0)

        @pl.when(u == 4 - near)
        def _():
            stats_columns(0)

        @pl.when(u == 5 - near)
        def _():
            stats_depth(0)

        forward((1, 2), u, lag_pair)

    stats_plane(0)
    for m in (1, 2):
        own_block(m)
    stats_rows(1)
    finish(0)
    gather_start(0)
    stats_columns(1)
    gather_step(0, 1)
    stats_depth(1)
    gather_step(0, 2)
    stats_plane(1)
    gather_step(0, 3)
    gather_step(0, 4)
    finish(1)
    for m in (1, 2):
        gather_start(m)
    gather_step(0, 5)
    for m in (1, 2):
        gather_step(m, 1)
    gather_step(0, 6)
    for m in (1, 2):
        gather_step(m, 2)
    gather_step(0, 7)
    for m in (1, 2):
        gather_step(m, 3)

    @pl.loop(4, 8)
    def _(s):
        for m in (1, 2):
            gather_step(m, s)

    @pl.loop(0, 8)
    def _(j):
        for m in range(3):

            @pl.when((near == 0) & (real(j, a) > 0))
            def _():
                for c in (0, 1):
                    raw_copy(m, real(j, a), c).wait_send()

            @pl.when((near >= 1) & (real(j, a) > near))
            def _():
                for c in (0, 1):
                    part_copy(m, a, near, real(j, a), c).wait_send()

            @pl.when(real(j, 1 - a) > far)
            def _():
                for c in (0, 1):
                    part_copy(m, 1 - a, far, real(j, 1 - a), c).wait_send()

            for d in (0, 1):
                held = (j <= k) if d == 0 else (j >= k)

                @pl.when(held & (k != 7 * (1 - d)))
                def _():
                    w_copy(m, d, j).wait_send()

    for b in (0, 1):
        for o in range(1, 4):
            y_copy(b, o).wait_send()
        for o in range(1, 8):
            p_copy(b, o).wait_send()

        @pl.loop(1, 16)
        def _(o):
            z_copy(b, o).wait_send()

        @pl.loop(1, 8)
        def _(o):
            f_copy(b, o).wait_send()

        @pl.loop(8, 32)
        def _(i):
            g_copy(b, i).wait_send()


def results_kernel(*refs):
    copies = [pltpu.make_async_copy(refs[i], refs[15 + i], refs[30].at[i]) for i in range(9)]
    for copy in copies:
        copy.start()
    for m in range(3):
        refs[24 + m][...] = refs[9 + m][0, 0 : HEIGHTS[m]]
        refs[27 + m][...] = refs[12 + m][0, :]
    for copy in copies:
        copy.wait()


def body(*args):
    grads = [args[4 * m].reshape(N, HEIGHTS[m], WIDTHS[m]) for m in range(3)]
    masters = [args[4 * m + 1] for m in range(3)]
    rows = [args[4 * m + 2] for m in range(3)]
    columns = [args[4 * m + 3] for m in range(3)]
    shape = jax.ShapeDtypeStruct
    blocks = list(zip(HEIGHTS, WIDTHS))
    out_shape = (
        [shape(b, F32) for b in blocks]
        + [shape((N, *b), BF16) for b in blocks]
        + [shape((1, 128), F32)] * 3
        + [shape((1, w), F32) for w in WIDTHS]
        + [shape(b, F32) for b in blocks]
    )
    vmem = pl.BlockSpec(memory_space=pltpu.VMEM)
    dma = pltpu.SemaphoreType.DMA
    out = pl.pallas_call(
        kernel,
        out_shape=out_shape,
        in_specs=[pl.BlockSpec(memory_space=pltpu.HBM)] * 12,
        out_specs=[vmem] * 15,
        scratch_shapes=(
            [pltpu.VMEM((2, N, *b), F32) for b in blocks]
            + [pltpu.VMEM((2, N, *b), BF16) for b in blocks]
            + [pltpu.VMEM(b, F32) for b in blocks]
            + [pltpu.VMEM((h, 128), F32) for h in HEIGHTS]
            + [
                pltpu.VMEM((2, 8, 128), F32),
                pltpu.VMEM((2, 4, 8, 128), F32),
                pltpu.VMEM((2, 8, 8, 128), F32),
                pltpu.VMEM((2, 8, 8, 128), F32),
                pltpu.VMEM((2, 8, 128), F32),
                pltpu.VMEM((2, 16, 8, 128), F32),
                pltpu.VMEM((2, 8, 128), F32),
                pltpu.VMEM((2, 8, 8, 128), F32),
                pltpu.VMEM((2, 32, 1, 128), F32),
                pltpu.VMEM((2, 8, 8, 128), F32),
                dma((3, 2, 8, 2)),
                dma((3, 2, 8, 2)),
                dma((3, 2, 8)),
                dma((3, 8)),
                dma((2, 2, 4)),
                dma((2, 2, 8)),
                dma((2, 2, 16)),
                dma((2, 2, 32)),
            ]
            + [pltpu.VMEM((N, *b), BF16) for b in blocks]
            + [pltpu.VMEM(b, F32) for b in blocks]
            + [pltpu.VMEM((h,), F32) for h in HEIGHTS]
            + [pltpu.VMEM((w,), F32) for w in WIDTHS]
            + [dma((12,))]
        ),
        compiler_params=pltpu.CompilerParams(
            collective_id=0, has_side_effects=True, vmem_limit_bytes=28 * 1024 * 1024
        ),
    )(*[pltpu.with_memory_space_constraint(v, pltpu.HBM) for v in (*grads, *masters, *rows, *columns)])
    anywhere = pl.BlockSpec(memory_space=pl.ANY)
    final_shape = (
        [shape(b, F32) for b in blocks]
        + [shape((N, *b), BF16) for b in blocks]
        + [shape(b, F32) for b in blocks]
        + [shape((h,), F32) for h in HEIGHTS]
        + [shape((w,), F32) for w in WIDTHS]
    )
    big = list(out[0:6]) + list(out[12:15])
    final = pl.pallas_call(
        results_kernel,
        out_shape=final_shape,
        in_specs=[vmem] * 15,
        out_specs=[anywhere] * 9 + [vmem] * 6,
        scratch_shapes=[dma((9,))],
        compiler_params=pltpu.CompilerParams(vmem_limit_bytes=8 * 1024 * 1024),
    )(*big, *out[6:12])
    result = []
    for m in range(3):
        result += [final[m], final[3 + m].reshape(N * HEIGHTS[m], WIDTHS[m]), final[9 + m], final[12 + m], final[6 + m]]
    return tuple(result)


def solution(mesh):
    finer = Mesh(mesh.devices.reshape(mesh.shape["dp"], 2, 4, 2, mesh.shape["col"]), ("dp", *ROW, "col"))
    one = (P("dp", ROW, "col"), P(ROW_DP, "col"), P(ROW_DP), P("col"))
    back = (P(ROW_DP, "col"), P(ROW, "col"), P(ROW_DP), P("col"), P(ROW_DP, "col"))
    return jax.shard_map(body, mesh=finer, in_specs=one * 3, out_specs=back * 3, check_vma=False)
```

```python
import jax
import jax.numpy as jnp
from jax import lax
from jax.experimental import pallas as pl
from jax.experimental.pallas import tpu as pltpu
from jax.sharding import Mesh
from jax.sharding import PartitionSpec as P

MESH = pl.DeviceIdType.MESH
F32 = jnp.float32
BF16 = jnp.bfloat16

ROW = ("zhi", "x", "core")
ROW_DP = ("zhi", "x", "core", "dp")

tiny_square = 1e-30
decay_rate = 0.9
learn_rate = 0.01

N = 8
HEIGHTS = (32, 40, 32)
WIDTHS = (1280, 1024, 1024)
FULL_ROWS = (4096, 5120, 4096)
FULL_COLS = (5120, 4096, 4096)
BATCHES = ((0,), (1, 2))
LAYOUT = (((0, 0, 0, 8), (1, 0, 8, 10)), ((0, 1, 0, 8), (1, 2, 0, 8)))


def remote(src, dst, send_sem, recv_sem, device):
    return pltpu.make_async_remote_copy(
        src_ref=src, dst_ref=dst, send_sem=send_sem, recv_sem=recv_sem, device_id=device, device_id_type=MESH
    )


def to_column(row, height):
    sub = lax.broadcasted_iota(jnp.int32, (height, 128), 0)
    lane = lax.broadcasted_iota(jnp.int32, (height, 128), 1)
    return jnp.sum(jnp.where(sub == lane, jnp.broadcast_to(row, (height, 128)), 0.0), axis=1, keepdims=True)


def to_row(column, height):
    sub = lax.broadcasted_iota(jnp.int32, (height, 128), 0)
    lane = lax.broadcasted_iota(jnp.int32, (height, 128), 1)
    return jnp.sum(jnp.where(sub == lane, jnp.broadcast_to(column, (height, 128)), 0.0), axis=0, keepdims=True)


def as_row(ref, height):
    return jnp.pad(ref[...].reshape(1, height), ((0, 0), (0, 128 - height)))


def kernel(*refs):
    given = refs[0:12]
    updated, weights, rows_next, columns_next, steps = refs[12:15], refs[15:18], refs[18:21], refs[21:24], refs[24:27]
    (
        part0, part1, part2, raw0, raw1, raw2, acc0, acc1, acc2,
        rfac0, rfac1, rfac2,
        ysend, yrecv, piece, pieces_in, zsend, zrecv, total, fin, ratios, colstat,
        rs_send, rs_recv, ag_send, ag_recv, y_sems, p_sems, z_sems, f_sems,
        *held, load_sems,
    ) = refs[27:]
    grads, masters, rows, columns = held[0:3], held[3:6], held[6:9], held[9:12]
    loads = [pltpu.make_async_copy(given[i], held[i], load_sems.at[i]) for i in range(12)]
    parts, raws, accs, rfacs = (part0, part1, part2), (raw0, raw1, raw2), (acc0, acc1, acc2), (rfac0, rfac1, rfac2)

    k = lax.axis_index("dp")
    zhi, x, core, y = lax.axis_index("zhi"), lax.axis_index("x"), lax.axis_index("core"), lax.axis_index("col")
    p = x * 2 + core
    q = zhi * 8 + k
    n = y * 8 + p

    def z_peer(o):
        t = lax.rem(q + o, 16)
        return {"zhi": t // 8, "dp": lax.rem(t, 8)}

    def p_peer(t):
        return {"x": t // 2, "core": lax.rem(t, 2)}

    def plane_peer(o):
        t = lax.rem(n + o, 32)
        s = lax.rem(t, 8)
        return {"x": s // 2, "core": lax.rem(s, 2), "col": t // 8}

    barrier = pltpu.get_barrier_semaphore()

    def far_first(i):
        return jnp.where(lax.rem(i, 2) == 1, 8 - (i + 1) // 2, 8 + i // 2)

    @pl.loop(0, 15)
    def _(i):
        pl.semaphore_signal(barrier, inc=1, device_id=z_peer(far_first(i)), device_id_type=MESH)

    @pl.loop(1, 32)
    def _(o):
        pl.semaphore_signal(barrier, inc=1, device_id=plane_peer(o), device_id_type=MESH)

    for load in loads:
        load.start()
    for load in loads:
        load.wait()
    pl.semaphore_wait(barrier, 46)

    a = k // 4
    near = jnp.where(a == 0, k, 7 - k)
    far = 7 - near

    def real(jd, d):
        return jd + d * (7 - 2 * jd)

    def half(m, c):
        return pl.ds(c * (WIDTHS[m] // 2), WIDTHS[m] // 2)

    def raw_copy(m, jd, c):
        j = real(jd, a)
        return remote(
            grads[m].at[j, :, half(m, c)], raws[m].at[a, j, :, half(m, c)], rs_send.at[m, a, j, c],
            rs_recv.at[m, a, j, c], {"dp": real(1, a)},
        )

    def part_copy(m, d, here, jd, c):
        j = real(jd, d)
        block = parts[m].at[d, j, :, half(m, c)]
        return remote(
            block, block, rs_send.at[m, d, j, c], rs_recv.at[m, d, j, c], {"dp": real(jnp.minimum(here + 1, 7), d)}
        )

    def send_raw(m):
        @pl.when(near == 0)
        def _():
            @pl.loop(0, 7)
            def _(s):
                for c in (0, 1):
                    raw_copy(m, 7 - s, c).start()

    def forward_first(m, jd, c):
        j = real(jd, a)
        cut = half(m, c)

        @pl.when((near == 1) & (jd > near))
        def _():
            raw_copy(m, jd, c).wait_recv()
            parts[m][a, j, :, cut] = raws[m][a, j, :, cut].astype(F32) + grads[m][j, :, cut].astype(F32)
            part_copy(m, a, near, jd, c).start()

        @pl.when((near >= 2) & (jd > near))
        def _():
            forward_part(m, a, near, jd, c)

    def forward_part(m, d, here, jd, c):
        j = real(jd, d)
        cut = half(m, c)
        part_copy(m, d, here, jd, c).wait_recv()
        parts[m][d, j, :, cut] = parts[m][d, j, :, cut] + grads[m][j, :, cut].astype(F32)
        part_copy(m, d, here, jd, c).start()

    def forward_second(m, r, c):
        @pl.when((r >= 0) & (7 - r > far))
        def _():
            forward_part(m, 1 - a, far, 7 - r, c)

    def forward(ms, u, behind):
        for m in ms:
            for c in (0, 1):
                forward_first(m, 7 - u, c)
                forward_second(m, u - behind, c)

    def own_block(m):
        b = 1 - a
        for c in (0, 1):
            part_copy(m, b, far, far, c).wait_recv()
        accs[m][...] = parts[m][b, k] + grads[m][k].astype(F32)

        @pl.when(near == 1)
        def _():
            for c in (0, 1):
                raw_copy(m, near, c).wait_recv()
            accs[m][...] = accs[m][...] + raws[m][a, k].astype(F32)

        @pl.when(near >= 2)
        def _():
            for c in (0, 1):
                part_copy(m, a, near, near, c).wait_recv()
            accs[m][...] = accs[m][...] + parts[m][a, k]

        accs[m][...] = accs[m][...] * 0.125

    def y_copy(b, o):
        t = lax.rem(y + o, 4)
        return remote(ysend.at[b], yrecv.at[b, o], y_sems.at[0, b, o], y_sems.at[1, b, o], {"col": t})

    def stats_rows(b):
        for at_row, m in enumerate(BATCHES[b]):
            square = accs[m][...] * accs[m][...] + tiny_square
            total_row = jnp.sum(square, axis=1, keepdims=True)
            ysend[b, at_row : at_row + 1] = to_row(total_row, HEIGHTS[m])
        for o in range(1, 4):
            y_copy(b, o).start()

    def p_copy(b, o):
        t = lax.rem(p + o, 8)
        return remote(piece.at[b, t], pieces_in.at[b, o], p_sems.at[0, b, o], p_sems.at[1, b, o], p_peer(t))

    def stats_columns(b):
        for o in range(1, 4):
            y_copy(b, o).wait_recv()
        piece[b] = jnp.zeros((8, 8, 128), F32)
        for m in BATCHES[b]:
            height = HEIGHTS[m]
            at = slice(BATCHES[b].index(m), BATCHES[b].index(m) + 1)
            across = (ysend[b, at] + yrecv[b, 1, at]) + (yrecv[b, 2, at] + yrecv[b, 3, at])
            new = decay_rate * as_row(rows[m], height) + (1.0 - decay_rate) * (across / FULL_COLS[m])
            rows_next[m][...] = new
            new_column = to_column(new, height)
            rfacs[m][...] = jnp.broadcast_to(new_column, (height, 128))
            row_sum = jnp.broadcast_to(jnp.sum(new_column, axis=0, keepdims=True), (1, 128))
            g = accs[m][...]
            square = g * g
            plain = jnp.sum(square + tiny_square, axis=0, keepdims=True)
            weighted = jnp.sum(square * (1.0 / new_column), axis=0, keepdims=True)
            for slot, owner, lo, hi in LAYOUT[b]:
                if owner != m:
                    continue
                for group in range(lo, hi):
                    cut = slice(128 * group, 128 * group + 128)
                    piece[b, group - lo, 2 * slot : 2 * slot + 1] = plain[:, cut]
                    piece[b, group - lo, 2 * slot + 1 : 2 * slot + 2] = weighted[:, cut]
            at_row = 7 - BATCHES[b].index(m)
            for which in range(8):
                piece[b, which, at_row : at_row + 1] = row_sum
        for o in range(1, 8):
            p_copy(b, o).start()

    def z_copy(b, o):
        return remote(zsend.at[b], zrecv.at[b, o], z_sems.at[0, b, o], z_sems.at[1, b, o], z_peer(o))

    def stats_depth(b):
        tile = piece[b, p]
        for o in range(1, 8):
            p_copy(b, o).wait_recv()
            tile = tile + pieces_in[b, o]
        zsend[b] = tile

        @pl.loop(0, 15)
        def _(i):
            z_copy(b, far_first(i)).start()

        colstat[b] = jnp.ones((8, 8, 128), F32)
        for slot, m, lo, hi in LAYOUT[b]:
            for group in range(lo, hi):
                cut = slice(128 * group, 128 * group + 128)
                colstat[b, group - lo, 2 * slot : 2 * slot + 1] = columns[m][cut].reshape(1, 128)

    def f_copy(b, o):
        t = lax.rem(p + o, 8)
        return remote(fin.at[b, p], fin.at[b, p], f_sems.at[0, b, o], f_sems.at[1, b, o], p_peer(t))

    def g_copy(b, i):
        t = lax.rem(p + lax.rem(i, 8), 8)
        peer = {"x": t // 2, "core": lax.rem(t, 2), "col": lax.rem(y + i // 8, 4)}
        return remote(ratios.at[b, 0], ratios.at[b, i], f_sems.at[0, b, i], f_sems.at[1, b, i], peer)

    def next_column(old, total_square, m):
        return decay_rate * old + (1.0 - decay_rate) * (total_square / FULL_ROWS[m])

    def stats_plane(b):
        @pl.loop(1, 16)
        def _(o):
            z_copy(b, o).wait_recv()

        tile = zsend[b]
        for o in range(1, 16):
            tile = tile + zrecv[b, o]
        total[b] = tile
        fin[b, p] = tile
        lane = lax.broadcasted_iota(jnp.int32, (1, 128), 1)
        marks = jnp.zeros((1, 128), F32)
        for slot, m, lo, hi in LAYOUT[b]:
            plain = total[b, 2 * slot : 2 * slot + 1]
            weighted = total[b, 2 * slot + 1 : 2 * slot + 2]
            new = next_column(colstat[b, p, 2 * slot : 2 * slot + 1], plain, m)
            ratio = jnp.sum(weighted / new, axis=1, keepdims=True)
            marks = marks + jnp.where(lane == slot, jnp.broadcast_to(ratio, (1, 128)), 0.0)
        ratios[b, 0] = marks
        fin[b, p, 5:6] = marks

        @pl.loop(0, 8)
        def _(o):
            g_copy(b, 16 + o).start()

        @pl.loop(0, 8)
        def _(o):
            g_copy(b, 8 + o).start()
            g_copy(b, 24 + o).start()

        @pl.loop(1, 8)
        def _(o):
            f_copy(b, o).start()

    def finish(b):
        @pl.loop(1, 8)
        def _(o):
            f_copy(b, o).wait_recv()

        @pl.loop(8, 32)
        def _(i):
            g_copy(b, i).wait_recv()

        everyone = fin[b, 0, 5:6]
        for which in range(1, 8):
            everyone = everyone + fin[b, which, 5:6]
        for which in range(8, 32):
            everyone = everyone + ratios[b, which]
        lane = lax.broadcasted_iota(jnp.int32, (1, 128), 1)
        for m in BATCHES[b]:
            for slot, owner, lo, hi in LAYOUT[b]:
                if owner != m:
                    continue
                for group in range(lo, hi):
                    cut = slice(128 * group, 128 * group + 128)
                    plain = fin[b, group - lo, 2 * slot : 2 * slot + 1]
                    columns_next[m][:, cut] = next_column(columns[m][cut].reshape(1, 128), plain, m)
            at_row = 7 - BATCHES[b].index(m)
            row_mean = total[b, at_row : at_row + 1] / FULL_ROWS[m]
            mine = [slot for slot, owner, _, _ in LAYOUT[b] if owner == m]
            chosen = lane == mine[0]
            for slot in mine[1:]:
                chosen = chosen | (lane == slot)
            ratio = jnp.sum(jnp.where(chosen, everyone, 0.0), axis=1, keepdims=True)
            mean_square = row_mean * ratio / (FULL_ROWS[m] * FULL_COLS[m])
            clip = jnp.maximum(1.0, jnp.sqrt(mean_square))
            row_scale = (jnp.sqrt(row_mean) / clip) / jnp.sqrt(rfacs[m][...])
            column_scale = 1.0 / jnp.sqrt(columns_next[m][...])
            step = accs[m][...] * row_scale[:, 0:1] * column_scale
            steps[m][...] = step
            new = masters[m][...] - learn_rate * step
            updated[m][...] = new
            weights[m][k] = new.astype(BF16)
            gather_start(m)

    def w_copy(m, d, i):
        to = jnp.clip(k + 1 - 2 * d, 0, 7)
        return remote(weights[m].at[i], weights[m].at[i], ag_send.at[m, d, i], ag_recv.at[m, i], {"dp": to})

    def gather_start(m):
        for d in (0, 1):

            @pl.when(k != 7 * (1 - d))
            def _():
                w_copy(m, d, k).start()

    def gather_step(m, s):
        for d in (0, 1):
            i = k - s if d == 0 else k + s

            @pl.when((i >= 0) & (i <= 7))
            def _():
                w_copy(m, d, i).wait_recv()

                @pl.when(k != 7 * (1 - d))
                def _():
                    w_copy(m, d, i).start()

    for m in range(3):
        send_raw(m)

    lag = jnp.where(near == 1, 6, jnp.where(near == 2, 4, 2))
    lag_pair = jnp.where(near == 1, 6, jnp.where(near == 2, 2, 1))

    @pl.loop(0, 8)
    def _(u):
        forward((0,), u, lag)

    @pl.loop(0, 8)
    def _(u):
        @pl.when(u == 3 - near)
        def _():
            own_block(0)
            stats_rows(0)

        @pl.when(u == 4 - near)
        def _():
            stats_columns(0)

        @pl.when(u == 5 - near)
        def _():
            stats_depth(0)

        forward((1, 2), u, lag_pair)

    stats_plane(0)
    for m in (1, 2):
        own_block(m)
    stats_rows(1)
    finish(0)
    stats_columns(1)
    gather_step(0, 1)
    stats_depth(1)
    gather_step(0, 2)
    stats_plane(1)
    gather_step(0, 3)
    gather_step(0, 4)
    finish(1)
    gather_step(0, 5)
    for m in (1, 2):
        gather_step(m, 1)
    gather_step(0, 6)
    for m in (1, 2):
        gather_step(m, 2)
    gather_step(0, 7)
    for m in (1, 2):
        gather_step(m, 3)

    @pl.loop(4, 8)
    def _(s):
        for m in (1, 2):
            gather_step(m, s)

    @pl.loop(0, 8)
    def _(j):
        for m in range(3):

            @pl.when((near == 0) & (real(j, a) > 0))
            def _():
                for c in (0, 1):
                    raw_copy(m, real(j, a), c).wait_send()

            @pl.when((near >= 1) & (real(j, a) > near))
            def _():
                for c in (0, 1):
                    part_copy(m, a, near, real(j, a), c).wait_send()

            @pl.when(real(j, 1 - a) > far)
            def _():
                for c in (0, 1):
                    part_copy(m, 1 - a, far, real(j, 1 - a), c).wait_send()

            for d in (0, 1):
                held = (j <= k) if d == 0 else (j >= k)

                @pl.when(held & (k != 7 * (1 - d)))
                def _():
                    w_copy(m, d, j).wait_send()

    for b in (0, 1):
        for o in range(1, 4):
            y_copy(b, o).wait_send()
        for o in range(1, 8):
            p_copy(b, o).wait_send()

        @pl.loop(1, 16)
        def _(o):
            z_copy(b, o).wait_send()

        @pl.loop(1, 8)
        def _(o):
            f_copy(b, o).wait_send()

        @pl.loop(8, 32)
        def _(i):
            g_copy(b, i).wait_send()


def results_kernel(*refs):
    copies = [pltpu.make_async_copy(refs[i], refs[15 + i], refs[30].at[i]) for i in range(9)]
    for copy in copies:
        copy.start()
    for m in range(3):
        refs[24 + m][...] = refs[9 + m][0, 0 : HEIGHTS[m]]
        refs[27 + m][...] = refs[12 + m][0, :]
    for copy in copies:
        copy.wait()


def body(*args):
    grads = [args[4 * m].reshape(N, HEIGHTS[m], WIDTHS[m]) for m in range(3)]
    masters = [args[4 * m + 1] for m in range(3)]
    rows = [args[4 * m + 2] for m in range(3)]
    columns = [args[4 * m + 3] for m in range(3)]
    shape = jax.ShapeDtypeStruct
    blocks = list(zip(HEIGHTS, WIDTHS))
    out_shape = (
        [shape(b, F32) for b in blocks]
        + [shape((N, *b), BF16) for b in blocks]
        + [shape((1, 128), F32)] * 3
        + [shape((1, w), F32) for w in WIDTHS]
        + [shape(b, F32) for b in blocks]
    )
    vmem = pl.BlockSpec(memory_space=pltpu.VMEM)
    dma = pltpu.SemaphoreType.DMA
    out = pl.pallas_call(
        kernel,
        out_shape=out_shape,
        in_specs=[pl.BlockSpec(memory_space=pltpu.HBM)] * 12,
        out_specs=[vmem] * 15,
        scratch_shapes=(
            [pltpu.VMEM((2, N, *b), F32) for b in blocks]
            + [pltpu.VMEM((2, N, *b), BF16) for b in blocks]
            + [pltpu.VMEM(b, F32) for b in blocks]
            + [pltpu.VMEM((h, 128), F32) for h in HEIGHTS]
            + [
                pltpu.VMEM((2, 8, 128), F32),
                pltpu.VMEM((2, 4, 8, 128), F32),
                pltpu.VMEM((2, 8, 8, 128), F32),
                pltpu.VMEM((2, 8, 8, 128), F32),
                pltpu.VMEM((2, 8, 128), F32),
                pltpu.VMEM((2, 16, 8, 128), F32),
                pltpu.VMEM((2, 8, 128), F32),
                pltpu.VMEM((2, 8, 8, 128), F32),
                pltpu.VMEM((2, 32, 1, 128), F32),
                pltpu.VMEM((2, 8, 8, 128), F32),
                dma((3, 2, 8, 2)),
                dma((3, 2, 8, 2)),
                dma((3, 2, 8)),
                dma((3, 8)),
                dma((2, 2, 4)),
                dma((2, 2, 8)),
                dma((2, 2, 16)),
                dma((2, 2, 32)),
            ]
            + [pltpu.VMEM((N, *b), BF16) for b in blocks]
            + [pltpu.VMEM(b, F32) for b in blocks]
            + [pltpu.VMEM((h,), F32) for h in HEIGHTS]
            + [pltpu.VMEM((w,), F32) for w in WIDTHS]
            + [dma((12,))]
        ),
        compiler_params=pltpu.CompilerParams(
            collective_id=0, has_side_effects=True, vmem_limit_bytes=28 * 1024 * 1024
        ),
    )(*[pltpu.with_memory_space_constraint(v, pltpu.HBM) for v in (*grads, *masters, *rows, *columns)])
    anywhere = pl.BlockSpec(memory_space=pl.ANY)
    final_shape = (
        [shape(b, F32) for b in blocks]
        + [shape((N, *b), BF16) for b in blocks]
        + [shape(b, F32) for b in blocks]
        + [shape((h,), F32) for h in HEIGHTS]
        + [shape((w,), F32) for w in WIDTHS]
    )
    big = list(out[0:6]) + list(out[12:15])
    final = pl.pallas_call(
        results_kernel,
        out_shape=final_shape,
        in_specs=[vmem] * 15,
        out_specs=[anywhere] * 9 + [vmem] * 6,
        scratch_shapes=[dma((9,))],
        compiler_params=pltpu.CompilerParams(vmem_limit_bytes=8 * 1024 * 1024),
    )(*big, *out[6:12])
    result = []
    for m in range(3):
        result += [final[m], final[3 + m].reshape(N * HEIGHTS[m], WIDTHS[m]), final[9 + m], final[12 + m], final[6 + m]]
    return tuple(result)


def solution(mesh):
    finer = Mesh(mesh.devices.reshape(mesh.shape["dp"], 2, 4, 2, mesh.shape["col"]), ("dp", *ROW, "col"))
    one = (P("dp", ROW, "col"), P(ROW_DP, "col"), P(ROW_DP), P("col"))
    back = (P(ROW_DP, "col"), P(ROW, "col"), P(ROW_DP), P("col"), P(ROW_DP, "col"))
    return jax.shard_map(body, mesh=finer, in_specs=one * 3, out_specs=back * 3, check_vma=False)
```
